32 devices in a mesh: gz: 8 (over z, x), gy: 4 (over y, core).
Axes of the slice: x: 2, y: 2, z: 4, core: 2. Of those that a mesh axis runs over, the one named last changes fastest.
Arguments:
- right_side: float32 [64, 32, 256], P('gz', 'gy'), may hold values from -10 to 10, as said below
Outputs:
- solution_field: float32 [64, 32, 256], P('gz', 'gy')
- residual: float32 [64, 32, 256], P('gz', 'gy')
The draws below stay inside these ranges and needn't reach their ends.
Inputs may be any that keep to these rules, and one draw needn't show every extreme that they name: `right_side`: a right-hand side.
All inputs are finite; a program needn't handle non-finite values.
Results may differ from the reference program's by a relative error of at most 0.00015.
Values sent between devices are 32-bit elements; how exact they have to be, the bound alone decides.
A program may use at most 64 MiB of HBM per device.

```python
import math
import jax
import jax.numpy as jnp

NX = 256
LEVELS = 3
NZ = 64
NY = 32


def draw_right_side(key, part):
    keys = jax.random.split(jax.random.fold_in(key, 11), 3)
    z_pos = jnp.arange(NZ, dtype=jnp.float32) / (NZ - 1)
    z_cell = jnp.arange(NZ, dtype=jnp.float32)[:, None, None]
    y_cell = jnp.arange(NY, dtype=jnp.float32)[None, :, None]
    x_cell = jnp.arange(NX, dtype=jnp.float32)[None, None, :]
    freqs = jax.random.uniform(keys[1], (4, 3), jnp.float32, 0.025, 0.1)
    phases = jax.random.uniform(keys[2], (4, 3), jnp.float32, 0.0, 2.0 * math.pi)
    smooth = jnp.zeros((NZ, NY, NX), jnp.float32)
    for term in range(4):
        smooth = smooth + 0.5 * (jnp.cos(2.0 * math.pi * freqs[term, 0] * z_cell + phases[term, 0]) * jnp.cos(2.0 * math.pi * freqs[term, 1] * y_cell + phases[term, 1]) * jnp.cos(2.0 * math.pi * freqs[term, 2] * x_cell + phases[term, 2]))
    smooth = jnp.clip(smooth, -2.0, 2.0)
    share = (0.15 + 0.85 * z_pos)[:, None, None]
    amplitude = jnp.exp(math.log(2.0) * z_pos)[:, None, None]
    noise = jnp.clip(jax.random.normal(keys[0], (NZ, NY, NX), jnp.float32), -3.5, 3.5)
    values = amplitude * (share * noise + (1.0 - share) * smooth)
    return jnp.clip(values, -10.0, 10.0).astype(jnp.float32)


def setup_inputs(seed: int = 0) -> dict:
    seeds = jax.random.split(jax.random.key(seed), 2)
    right_side = draw_right_side(jax.random.fold_in(seeds[1], 71), 0)
    return dict(right_side=right_side)


sweep_order = [((0, 0), (0, 1)), ((0, 1), (0, 1)), ((1, 0), (0, 1)), ((1, 1), (0, 1)),
               ((1, 1), (1, 0)), ((1, 0), (1, 0)), ((0, 1), (1, 0)), ((0, 0), (1, 0))]


def x_side(field):
    width = [(0, 0)] * (field.ndim - 1)
    upper = jnp.pad(field[..., 1:], width + [(0, 1)])
    lower = jnp.pad(field[..., :-1], width + [(1, 0)])
    return upper + lower


def operate(padded):
    z_cells = padded.shape[0] - 2
    y_cells = padded.shape[1] - 2
    boxed = jnp.zeros((z_cells, y_cells, padded.shape[2]), jnp.float32)
    for z_step in range(3):
        for y_step in range(3):
            boxed = boxed + padded[z_step:z_step + z_cells, y_step:y_step + y_cells, :]
    boxed = boxed + x_side(boxed)
    return 27.0 * padded[1:-1, 1:-1, :] - boxed


def group_update(padded, rhs, z_par, y_par, x_order):
    z_cells = padded.shape[0] - 2
    y_cells = padded.shape[1] - 2
    outer = None
    for z_step in (-1, 0, 1):
        for y_step in (-1, 0, 1):
            if z_step == 0 and y_step == 0:
                continue
            row = padded[1 + z_par + z_step:z_cells + z_par + z_step:2, 1 + y_par + y_step:y_cells + y_par + y_step:2, :]
            outer = row if outer is None else outer + row
    center = padded[1 + z_par:z_cells + z_par:2, 1 + y_par:y_cells + y_par:2, :]
    total = outer + x_side(outer) + rhs[z_par::2, y_par::2, :]
    parity = jnp.arange(padded.shape[2], dtype=jnp.int32) % 2
    for x_par in x_order:
        center = jnp.where(parity == x_par, (total + x_side(center)) / 26.0, center)
    return padded.at[1 + z_par:z_cells + z_par:2, 1 + y_par:y_cells + y_par:2, :].set(center)


def pad_zero(field):
    return jnp.pad(field, ((1, 1), (1, 1), (0, 0)))


def symmetric_sweeps(rhs, start):
    padded = pad_zero(start)
    for group, x_order in sweep_order:
        padded = group_update(padded, rhs, group[0], group[1], x_order)
    return padded[1:-1, 1:-1, :]


def vcycle(rhs, level):
    zeros = jnp.zeros_like(rhs)
    if level == LEVELS - 1:
        return symmetric_sweeps(rhs, zeros)
    first = symmetric_sweeps(rhs, zeros)
    defect = rhs - operate(pad_zero(first))
    coarse = vcycle(defect[::2, ::2, ::2], level + 1)
    return symmetric_sweeps(rhs, first.at[::2, ::2, ::2].add(coarse))


def reference(right_side):
    precond = vcycle(right_side, 0)
    image = operate(pad_zero(precond))
    alpha = jnp.sum(right_side * precond) / jnp.sum(precond * image)
    return alpha * precond, right_side - alpha * image
```

```python
import functools

import jax
import jax.numpy as jnp
from jax import lax
from jax.experimental import pallas as pl
from jax.experimental.pallas import tpu as pltpu
from jax.sharding import PartitionSpec as P

MESH = pl.DeviceIdType.MESH
F32 = jnp.float32

LOW0, LOW1, LOW2 = 4, 6, 2
EVENS, ODDS = 9, 8
WINDOW = EVENS + ODDS

PHASE_A = ((0, (0, 1)), (1, (0, 1)))
PHASE_B = ((0, (0, 1)), (1, (0, 1, 0)), (0, (1, 0)))
PHASE_C = ((1, (1, 0)), (0, (1, 0)))

CHUNK0 = 3
CHUNK1 = 9


def add(*terms):
    total = None
    for term in terms:
        if term is not None:
            total = term if total is None else total + term
    return total


def shift(x, axis, step):
    if x is None:
        return None
    size = x.shape[axis]
    moved = pltpu.roll(x, step % size, axis)
    index = lax.broadcasted_iota(jnp.int32, x.shape, axis)
    keep = index >= step if step > 0 else index < size + step
    return jnp.where(keep, moved, 0.0)


def pair_sum(other, parity, axis):
    return add(other, shift(other, axis, 1 if parity == 0 else -1))


def both_sides(x, axis, step):
    return add(shift(x, axis, step), shift(x, axis, -step))


def scale_rows(shape, first, count):
    row = first + 2 * lax.broadcasted_iota(jnp.int32, shape, 0)
    return jnp.where((row >= 0) & (row < count), F32(1.0 / 26.0), F32(0.0))


def box0(s):
    tall = [[add(s[yp][xp], pair_sum(s[1 - yp][xp], yp, 1)) for xp in (0, 1)] for yp in (0, 1)]
    return [[add(tall[yp][xp], pair_sum(tall[yp][1 - xp], xp, 2)) for xp in (0, 1)] for yp in (0, 1)]


def edge_twice(x, axis, width, at_end):
    size = x.shape[axis]
    index = lax.broadcasted_iota(jnp.int32, x.shape, axis)
    inner = index < size - width if at_end else index >= width
    return x * jnp.where(inner, F32(2.0), F32(1.0))


def phase0(v, f, zs, scale, steps):
    v = [list(v[0]), list(v[1])]
    for yp, order in steps:
        w = [add(zs[yp][xp], pair_sum(add(zs[1 - yp][xp], v[1 - yp][xp]), yp, 1)) for xp in (0, 1)]
        a, b = order[0], order[1]
        near, far = (1, -1) if a == 0 else (-1, 1)
        u = add(w[b], v[yp][b])
        h = add(f[yp][a], w[a])
        q = add(w[a], h * scale)
        u_near = shift(u, 2, near)
        v[yp][a] = add(h, u, u_near) * scale
        twice = None if u is None else add(edge_twice(u, 2, 1, a == 0), u_near, shift(u, 2, far)) * scale
        v[yp][b] = add(f[yp][b], w[b], q, shift(q, 2, far), twice) * scale
        if len(order) == 3:
            v[yp][a] = add(h, pair_sum(add(w[b], v[yp][b]), a, 2)) * scale
    return v


def box1(s):
    tall = [add(s[yp], pair_sum(s[1 - yp], yp, 1)) for yp in (0, 1)]
    return [add(t, both_sides(t, 2, 1)) for t in tall]


def line_pair(v, g, w, scale, parity, order, step):
    a, b = order[0], order[1]
    first = parity == a
    h = add(g, w)
    u = add(w, v)
    m = jnp.where(first, add(w, h * scale), 0.0 if u is None else u)
    second = add(edge_twice(m, 2, step, b == 1), both_sides(m, 2, 2 * step)) * jnp.where(first, F32(0.0), scale)
    new = add(h, both_sides(m, 2, step), second) * scale
    if len(order) == 3:
        new = jnp.where(first, add(h, both_sides(add(w, new), 2, step)) * scale, new)
    return new


def phase1(v, g, zs, scale, steps):
    v = list(v)
    parity = lax.broadcasted_iota(jnp.int32, scale.shape, 2) % 2
    for yp, order in steps:
        w = add(zs[yp], pair_sum(add(zs[1 - yp], v[1 - yp]), yp, 1))
        v[yp] = line_pair(v[yp], g[yp], w, scale, parity, order, 1)
    return v


def phase2(v, g, zs, scale, steps):
    shape = scale.shape
    y_par = lax.broadcasted_iota(jnp.int32, shape, 1) % 2
    x_par = (lax.broadcasted_iota(jnp.int32, shape, 2) // 2) % 2
    for yp, order in steps:
        w = add(zs, both_sides(add(zs, v), 1, 1))
        new = line_pair(v, g, w, scale, x_par, order, 2)
        v = jnp.where(y_par == yp, new, 0.0 if v is None else v)
    return v


def chunks(low, high, size):
    for start in range(low, high, size):
        yield start, min(size, high - start)


YX = [(0, 0), (0, 1), (1, 0), (1, 1)]


NONE = [[None, None], [None, None]]


def run0(v, f, z0, z_count, odd, low, high, steps, fresh):
    for at, n in chunks(low, high, CHUNK0):
        here = pl.ds(at, n)
        below, above = (pl.ds(at, n), pl.ds(at + 1, n)) if odd else (pl.ds(at - 1, n), pl.ds(at, n))
        rhs = [[f[odd][yp, xp, here] for xp in (0, 1)] for yp in (0, 1)]
        scale = scale_rows(rhs[0][0].shape, z0 + 2 * at - LOW0 + odd, z_count)
        zs, old = NONE, NONE
        if fresh > 0:
            zs = [[v[1 - odd][yp, xp, below] + v[1 - odd][yp, xp, above] for xp in (0, 1)] for yp in (0, 1)]
        if fresh > 1:
            old = [[v[odd][yp, xp, here] for xp in (0, 1)] for yp in (0, 1)]
        new = phase0(old, rhs, zs, scale, steps)
        for yp, xp in YX:
            v[odd][yp, xp, here] = new[yp][xp]


def run1(v, f, z0, z_count, odd, low, high, steps, fresh):
    for at, n in chunks(low, high, CHUNK1):
        here = pl.ds(at, n)
        below, above = (pl.ds(at, n), pl.ds(at + 1, n)) if odd else (pl.ds(at - 1, n), pl.ds(at, n))
        g = [f[here, odd, yp] for yp in (0, 1)]
        scale = scale_rows(g[0].shape, z0 + 2 * at - LOW1 + odd, z_count)
        zs, old = NONE[0], NONE[0]
        if fresh > 0:
            zs = [v[1 - odd][yp, below] + v[1 - odd][yp, above] for yp in (0, 1)]
        if fresh > 1:
            old = [v[odd][yp, here] for yp in (0, 1)]
        new = phase1(old, g, zs, scale, steps)
        for yp in (0, 1):
            v[odd][yp, here] = new[yp]


def permutation(size, inverse):
    half = size // 2
    wide = lax.broadcasted_iota(jnp.int32, (size, size), 0 if inverse else 1)
    tall = lax.broadcasted_iota(jnp.int32, (size, size), 1 if inverse else 0)
    source = jnp.where(wide < half, 2 * wide, 2 * (wide - half) + 1)
    return jnp.where(tall == source, F32(1.0), F32(0.0))


def kernel(
    gz_n, gy_n, rhs_hbm, sol_ref, res_ref,
    flat, mine, got, fe, fo, ve, vo, dbuf, f1, v1e, v1o, vc, part, parts, nat,
    ssem, r1, r2, r3, rhs_ref, s5, token,
):
    gz, gy = lax.axis_index("gz"), lax.axis_index("gy")
    zl, yl, nx = rhs_ref.shape
    fetch = pltpu.make_async_copy(rhs_hbm, rhs_ref, s5)
    fetch.start()
    y2, x2 = yl // 2, nx // 2
    yc = y2 // 2
    zc = zl // 2
    z_count = gz_n * zl
    z0 = gz * zl
    f, v = (fe, fo), (ve, vo)
    v1 = (v1e, v1o)
    halves = gy_n // 2
    sibling = gy + 1 - 2 * lax.rem(gy, 2)

    def there(dz):
        return (gz + dz >= 0) & (gz + dz < gz_n)

    def when_there(dz, go):
        if dz == 0:
            go()
        else:
            pl.when(there(dz))(go)

    barrier = pltpu.get_barrier_semaphore()
    count = jnp.int32(0)
    greet = [(0, dg) for dg in range(1, gy_n)] + [(dz, 2 * h) for dz in (-1, 1) for h in range(halves)] + [(-2, 0), (2, 0)]
    for dz, dg in greet:

        def go(dz=dz, dg=dg):
            pl.semaphore_signal(
                barrier, inc=1, device_id=(gz + dz, lax.rem(gy + dg, gy_n)), device_id_type=MESH
            )

        when_there(dz, go)
        count = count + (1 if dz == 0 else there(dz).astype(jnp.int32))

    fetch.wait()
    split = jnp.dot(
        rhs_ref[...].reshape(zl * yl, nx), permutation(nx, False),
        precision=lax.Precision.HIGHEST, preferred_element_type=F32,
    )
    for xp in (0, 1):
        flat[xp] = split[:, xp * x2 : (xp + 1) * x2]
    for z in range(zl):
        for yp, xp in YX:
            row = flat[xp, pl.ds(z * yl + yp, y2, stride=2), :]
            mine[z, (yp * 2 + xp) * y2 : (yp * 2 + xp + 1) * y2, :] = row
    got[gy, pl.ds(LOW0, zl)] = mine[...]

    @pl.when(gz == 0)
    def _():
        got[:, 0:LOW0] = jnp.zeros((gy_n, LOW0) + got.shape[2:], F32)

    @pl.when(gz == gz_n - 1)
    def _():
        got[:, LOW0 + zl :] = jnp.zeros((gy_n, WINDOW - LOW0 - zl) + got.shape[2:], F32)

    high = WINDOW - LOW0 - zl
    moves1 = {-1: (0, high, LOW0 + zl), 0: (0, zl, LOW0), 1: (zl - LOW0, LOW0, 0)}
    moves2 = {-2: (0, zc // 2, 7), -1: (0, zc // 2, 5), 1: (0, zc // 2, 1), 2: (zc // 2 - 1, 1, 0)}

    order1 = [
        (slot, dz, h) for h in range(halves) for slot, dz in ((2, 0), (0, 1), (1, -1)) if dz != 0 or h != 0
    ]

    def pass_token(round_):
        reach = 2 << round_
        for dz in (-reach, reach):
            when_there(dz, lambda dz=dz: pl.semaphore_signal(
                token.at[round_], inc=1, device_id=(gz + dz, gy), device_id_type=MESH
            ))

    def take_token(round_):
        reach = 2 << round_
        pl.semaphore_wait(token.at[round_], there(-reach).astype(jnp.int32) + there(reach).astype(jnp.int32))

    def gather():
        def blocks(act):
            for slot, dz in enumerate((1, -1, 0)):
                for h in range(halves):
                    if dz == 0 and h == 0:
                        continue
                    act(slot, dz, h)

        def direct(slot, dz, h, owner):
            first, n, to = moves1[dz]
            g = lax.rem(gy + 2 * h, gy_n)
            return pltpu.make_async_remote_copy(
                src_ref=mine.at[pl.ds(first, n)],
                dst_ref=got.at[g if owner else gy, pl.ds(to, n)],
                send_sem=ssem.at[slot * halves + h],
                recv_sem=r1.at[slot, g if owner else gy],
                device_id=(gz - dz if owner else gz + dz, g),
                device_id_type=MESH,
            )

        def relay(slot, dz, h, owner):
            _, n, to = moves1[dz]
            g = lax.rem((sibling if owner else gy) + 2 * h, gy_n)
            place = got.at[g, pl.ds(to, n)]
            return pltpu.make_async_remote_copy(
                src_ref=mine if dz == 0 and h == 0 else place,
                dst_ref=place,
                send_sem=ssem.at[(3 + slot) * halves + h],
                recv_sem=r1.at[slot, g],
                device_id=(gz, sibling),
                device_id_type=MESH,
            )

        blocks(lambda slot, dz, h: when_there(dz, lambda: direct(slot, dz, h, False).start()))
        relay(2, 0, 0, False).start()

        def forward(slot, dz, h):
            def go():
                direct(slot, dz, h, True).wait_recv()
                relay(slot, dz, h, False).start()

            when_there(-dz, go)

        for slot, dz, h in order1:
            forward(slot, dz, h)
        for r in range(min(rounds, 1)):
            take_token(r)
            if r + 1 < rounds:
                pass_token(r + 1)
        relay(2, 0, 0, True).wait_recv()
        for slot, dz, h in order1:
            when_there(-dz, lambda: relay(slot, dz, h, True).wait_recv())
        relay(2, 0, 0, False).wait_send()
        for slot, dz, h in order1:
            when_there(-dz, lambda: relay(slot, dz, h, False).wait_send())
        blocks(lambda slot, dz, h: when_there(dz, lambda: direct(slot, dz, h, False).wait_send()))

    rounds = max(gz_n - 2, 1).bit_length() - 1
    pl.semaphore_wait(barrier, count)
    if rounds > 0:
        pass_token(0)
    gather()

    for q in range(WINDOW):
        for k, (yp, xp) in enumerate(YX):
            for g in range(gy_n):
                f[q % 2][yp, xp, q // 2, g * y2 : (g + 1) * y2, :] = got[g, q, k * y2 : (k + 1) * y2, :]

    run0(v, f, z0, z_count, 0, 0, EVENS, PHASE_A, 0)
    run0(v, f, z0, z_count, 1, 0, ODDS, PHASE_B, 1)
    run0(v, f, z0, z_count, 0, 1, EVENS - 1, PHASE_C, 2)

    own = LOW0 // 2
    here, below, above = pl.ds(own, zc), pl.ds(own - 1, zc), pl.ds(own, zc)
    s = [[ve[yp, xp, here] + vo[yp, xp, below] + vo[yp, xp, above] for xp in (0, 1)] for yp in (0, 1)]
    tall = [s[0][xp] + pair_sum(s[1][xp], 0, 1) for xp in (0, 1)]
    dbuf[...] = fe[0, 0, here] - (27.0 * ve[0, 0, here] - (tall[0] + pair_sum(tall[1], 0, 2)))
    half = gy_n * yc
    for z in range(zc):
        for yp in (0, 1):
            f1[3 + z // 2, z % 2, yp] = dbuf[z, pl.ds(yp, half, stride=2), :]
    for edge, low, n in ((0, 0, 3), (1, 0, 1), (gz_n - 2, 7, 2), (gz_n - 1, 5, 4)):

        @pl.when(gz == edge)
        def _(low=low, n=n):
            f1[low : low + n] = jnp.zeros((n,) + f1.shape[1:], F32)

    def near(slot, dz):
        first, n, to = moves2[dz]
        return pltpu.make_async_remote_copy(
            src_ref=f1.at[pl.ds(3 + first, n)], dst_ref=f1.at[pl.ds(to, n)],
            send_sem=ssem.at[slot], recv_sem=r2.at[slot],
            device_id=(gz + dz, gy), device_id_type=MESH,
        )

    far_first = sorted(moves2, key=lambda d: -abs(d))
    for slot, dz in enumerate(far_first):
        when_there(dz, lambda: near(slot, dz).start())
    for slot, dz in enumerate(far_first):
        when_there(-dz, lambda: near(slot, dz).wait_recv())
    for slot, dz in enumerate(far_first):
        when_there(dz, lambda: near(slot, dz).wait_send())

    for r in range(1, rounds):
        take_token(r)
        if r + 1 < rounds:
            pass_token(r + 1)

    c0, c_count = gz * zc, gz_n * zc
    run1(v1, f1, c0, c_count, 0, 0, EVENS, PHASE_A, 0)
    run1(v1, f1, c0, c_count, 1, 0, ODDS, PHASE_B, 1)
    run1(v1, f1, c0, c_count, 0, 1, EVENS - 1, PHASE_C, 2)

    f2 = []
    for i in range(1, EVENS - 1):
        s = [v1e[yp, pl.ds(i, 1)] + v1o[yp, pl.ds(i - 1, 1)] + v1o[yp, pl.ds(i, 1)] for yp in (0, 1)]
        tall = s[0] + pair_sum(s[1], 0, 1)
        f2.append(f1[pl.ds(i, 1), 0, 0] - (27.0 * v1e[0, pl.ds(i, 1)] - (tall + both_sides(tall, 2, 1))))
    q0, q_count = gz * (zc // 2), gz_n * (zc // 2)
    f2e, f2o = f2[0::2], f2[1::2]
    scale2 = [scale_rows(f2[0].shape, q0 - LOW2 + i, q_count) for i in range(7)]
    even2 = [phase2(None, f2e[k], None, scale2[2 * k], PHASE_A) for k in range(4)]
    odd2 = [phase2(None, f2o[k], even2[k] + even2[k + 1], scale2[2 * k + 1], PHASE_B) for k in range(3)]
    for k in (1, 2):
        even2[k] = phase2(even2[k], f2e[k], odd2[k - 1] + odd2[k], scale2[2 * k], PHASE_C)
    v2 = [odd2[0], even2[1], odd2[1], even2[2], odd2[2]]
    in_lane = lax.broadcasted_iota(jnp.int32, v2[0].shape, 2) % 2 == 0
    for k in range(5):
        v1e[0, pl.ds(2 + k, 1)] = v1e[0, pl.ds(2 + k, 1)] + jnp.where(in_lane, v2[k], 0.0)

    run1(v1, f1, c0, c_count, 0, 2, 7, PHASE_A, 2)
    run1(v1, f1, c0, c_count, 1, 2, 6, PHASE_B, 2)
    run1(v1, f1, c0, c_count, 0, 3, 6, PHASE_C, 2)

    for c in range(-1, 6):
        odd = c % 2
        i = (c + LOW1 - odd) // 2
        for yp in (0, 1):
            vc[c + 1, pl.ds(yp, half, stride=2), :] = v1[odd][yp, i]
    ve[0, 0, pl.ds(1, 7)] = ve[0, 0, pl.ds(1, 7)] + vc[...]

    run0(v, f, z0, z_count, 0, 1, 8, PHASE_A, 2)
    run0(v, f, z0, z_count, 1, 1, 7, PHASE_B, 2)
    run0(v, f, z0, z_count, 0, 2, 7, PHASE_C, 2)

    numer = denom = None
    for odd in (0, 1):
        for k in range(zc):
            i = own + k
            here, below, above = pl.ds(i, 1), pl.ds(i - 1 + odd, 1), pl.ds(i + odd, 1)
            p = [[v[odd][yp, xp, here] for xp in (0, 1)] for yp in (0, 1)]
            s = [[p[yp][xp] + v[1 - odd][yp, xp, below] + v[1 - odd][yp, xp, above] for xp in (0, 1)] for yp in (0, 1)]
            b = box0(s)
            for yp, xp in YX:
                image = 27.0 * p[yp][xp] - b[yp][xp]
                numer = add(numer, f[odd][yp, xp, here] * p[yp][xp])
                denom = add(denom, p[yp][xp] * image)
                parity_at = k * 2 + odd
                nat[yp, xp, pl.ds(parity_at, 1)] = image
    rows = numer.shape[1]
    for j, total in enumerate((numer, denom)):
        acc = None
        for r in range(0, rows, 8):
            acc = add(acc, total[0, r : r + 8, :])
        part[pl.ds(j, 1), :] = jnp.sum(acc, axis=0, keepdims=True)

    sends, receives = [], []
    for d in range(1, gz_n):
        to = lax.rem(gz + d, gz_n)
        sends.append(pltpu.make_async_remote_copy(
            src_ref=part, dst_ref=parts.at[gz], send_sem=ssem.at[d - 1], recv_sem=r3.at[gz],
            device_id=(to, gy), device_id_type=MESH,
        ))
        receives.append(pltpu.make_async_remote_copy(
            src_ref=part, dst_ref=parts.at[to], send_sem=ssem.at[d - 1], recv_sem=r3.at[to],
            device_id=(to, gy), device_id_type=MESH,
        ))
    for c in sends:
        c.start()
    parts[gz] = part[...]

    back = permutation(nx, True)
    for which, out in ((0, sol_ref), (1, res_ref)):
        for z in range(zl):
            for yp, xp in YX:
                if which == 0:
                    row = v[z % 2][yp, xp, own + z // 2, pl.ds(gy * y2, y2), :]
                else:
                    row = nat[yp, xp, z, pl.ds(gy * y2, y2), :]
                flat[xp, pl.ds(z * yl + yp, y2, stride=2), :] = row
        out[...] = jnp.dot(
            jnp.concatenate([flat[0], flat[1]], axis=1), back, precision=lax.Precision.HIGHEST, preferred_element_type=F32
        ).reshape(zl, yl, nx)

    for c in receives:
        c.wait_recv()
    for c in sends:
        c.wait_send()
    sums = parts[0]
    for d in range(1, gz_n):
        sums = sums + parts[d]
    alpha = jnp.sum(sums[0:1], axis=1, keepdims=True) / jnp.sum(sums[1:2], axis=1, keepdims=True)
    alpha = alpha.reshape(1, 1, 1)
    sol_ref[...] = sol_ref[...] * alpha
    res_ref[...] = rhs_ref[...] - res_ref[...] * alpha


def solution(mesh):
    gz_n, gy_n = mesh.shape["gz"], mesh.shape["gy"]

    def body(rhs):
        zl, yl, nx = rhs.shape
        y2, x2 = yl // 2, nx // 2
        y_half = gy_n * y2
        zc, yc = zl // 2, y2 // 2
        vmem = lambda *shape: pltpu.VMEM(shape, F32)
        dma = lambda *shape: pltpu.SemaphoreType.DMA(shape)
        return pl.pallas_call(
            functools.partial(kernel, gz_n, gy_n),
            out_shape=[vmem(*rhs.shape)] * 2,
            in_specs=[pl.BlockSpec(memory_space=pl.ANY)],
            out_specs=[pl.BlockSpec(memory_space=pltpu.VMEM)] * 2,
            scratch_shapes=[
                vmem(2, zl * yl, x2),
                vmem(zl, 4 * y2, x2),
                vmem(gy_n, WINDOW, 4 * y2, x2),
                vmem(2, 2, EVENS, y_half, x2),
                vmem(2, 2, ODDS, y_half, x2),
                vmem(2, 2, EVENS, y_half, x2),
                vmem(2, 2, ODDS, y_half, x2),
                vmem(zc, y_half, x2),
                vmem(9, 2, 2, gy_n * yc, x2),
                vmem(2, EVENS, gy_n * yc, x2),
                vmem(2, ODDS, gy_n * yc, x2),
                vmem(7, y_half, x2),
                vmem(2, x2),
                vmem(gz_n, 2, x2),
                vmem(2, 2, zl, y_half, x2),
                dma(max(6 * (gy_n // 2), gz_n)), dma(3, gy_n), dma(4), dma(gz_n),
                vmem(zl, yl, nx), pltpu.SemaphoreType.DMA,
                pltpu.SemaphoreType.REGULAR((max(1, max(gz_n - 2, 1).bit_length() - 1),)),
            ],
            compiler_params=pltpu.CompilerParams(has_side_effects=True, collective_id=0),
        )(rhs)

    return jax.shard_map(
        lambda rhs: tuple(body(rhs)),
        mesh=mesh,
        in_specs=(P("gz", "gy", None),),
        out_specs=(P("gz", "gy", None), P("gz", "gy", None)),
        check_vma=False,
    )
```

```python
import functools

import jax
import jax.numpy as jnp
from jax import lax
from jax.experimental import pallas as pl
from jax.experimental.pallas import tpu as pltpu
from jax.sharding import PartitionSpec as P

MESH = pl.DeviceIdType.MESH
F32 = jnp.float32

LOW0, LOW1, LOW2 = 4, 6, 2
EVENS, ODDS = 9, 8
WINDOW = EVENS + ODDS

PHASE_A = ((0, (0, 1)), (1, (0, 1)))
PHASE_B = ((0, (0, 1)), (1, (0, 1, 0)), (0, (1, 0)))
PHASE_C = ((1, (1, 0)), (0, (1, 0)))

CHUNK0 = 3
CHUNK1 = 9


def add(*terms):
    total = None
    for term in terms:
        if term is not None:
            total = term if total is None else total + term
    return total


def shift(x, axis, step):
    if x is None:
        return None
    size = x.shape[axis]
    moved = pltpu.roll(x, step % size, axis)
    index = lax.broadcasted_iota(jnp.int32, x.shape, axis)
    keep = index >= step if step > 0 else index < size + step
    return jnp.where(keep, moved, 0.0)


def pair_sum(other, parity, axis):
    return add(other, shift(other, axis, 1 if parity == 0 else -1))


def both_sides(x, axis, step):
    return add(shift(x, axis, step), shift(x, axis, -step))


def scale_rows(shape, first, count):
    row = first + 2 * lax.broadcasted_iota(jnp.int32, shape, 0)
    return jnp.where((row >= 0) & (row < count), F32(1.0 / 26.0), F32(0.0))


def box0(s):
    tall = [[add(s[yp][xp], pair_sum(s[1 - yp][xp], yp, 1)) for xp in (0, 1)] for yp in (0, 1)]
    return [[add(tall[yp][xp], pair_sum(tall[yp][1 - xp], xp, 2)) for xp in (0, 1)] for yp in (0, 1)]


def edge_twice(x, axis, width, at_end):
    size = x.shape[axis]
    index = lax.broadcasted_iota(jnp.int32, x.shape, axis)
    inner = index < size - width if at_end else index >= width
    return x * jnp.where(inner, F32(2.0), F32(1.0))


def phase0(v, f, zs, scale, steps):
    v = [list(v[0]), list(v[1])]
    for yp, order in steps:
        w = [add(zs[yp][xp], pair_sum(add(zs[1 - yp][xp], v[1 - yp][xp]), yp, 1)) for xp in (0, 1)]
        a, b = order[0], order[1]
        near, far = (1, -1) if a == 0 else (-1, 1)
        u = add(w[b], v[yp][b])
        h = add(f[yp][a], w[a])
        q = add(w[a], h * scale)
        u_near = shift(u, 2, near)
        v[yp][a] = add(h, u, u_near) * scale
        twice = None if u is None else add(edge_twice(u, 2, 1, a == 0), u_near, shift(u, 2, far)) * scale
        v[yp][b] = add(f[yp][b], w[b], q, shift(q, 2, far), twice) * scale
        if len(order) == 3:
            v[yp][a] = add(h, pair_sum(add(w[b], v[yp][b]), a, 2)) * scale
    return v


def box1(s):
    tall = [add(s[yp], pair_sum(s[1 - yp], yp, 1)) for yp in (0, 1)]
    return [add(t, both_sides(t, 2, 1)) for t in tall]


def line_pair(v, g, w, scale, parity, order, step):
    a, b = order[0], order[1]
    first = parity == a
    h = add(g, w)
    u = add(w, v)
    m = jnp.where(first, add(w, h * scale), 0.0 if u is None else u)
    second = add(edge_twice(m, 2, step, b == 1), both_sides(m, 2, 2 * step)) * jnp.where(first, F32(0.0), scale)
    new = add(h, both_sides(m, 2, step), second) * scale
    if len(order) == 3:
        new = jnp.where(first, add(h, both_sides(add(w, new), 2, step)) * scale, new)
    return new


def phase1(v, g, zs, scale, steps):
    v = list(v)
    parity = lax.broadcasted_iota(jnp.int32, scale.shape, 2) % 2
    for yp, order in steps:
        w = add(zs[yp], pair_sum(add(zs[1 - yp], v[1 - yp]), yp, 1))
        v[yp] = line_pair(v[yp], g[yp], w, scale, parity, order, 1)
    return v


def phase2(v, g, zs, scale, steps):
    shape = scale.shape
    y_par = lax.broadcasted_iota(jnp.int32, shape, 1) % 2
    x_par = (lax.broadcasted_iota(jnp.int32, shape, 2) // 2) % 2
    for yp, order in steps:
        w = add(zs, both_sides(add(zs, v), 1, 1))
        new = line_pair(v, g, w, scale, x_par, order, 2)
        v = jnp.where(y_par == yp, new, 0.0 if v is None else v)
    return v


def chunks(low, high, size):
    for start in range(low, high, size):
        yield start, min(size, high - start)


YX = [(0, 0), (0, 1), (1, 0), (1, 1)]


NONE = [[None, None], [None, None]]


def run0(v, f, z0, z_count, odd, low, high, steps, fresh):
    for at, n in chunks(low, high, CHUNK0):
        here = pl.ds(at, n)
        below, above = (pl.ds(at, n), pl.ds(at + 1, n)) if odd else (pl.ds(at - 1, n), pl.ds(at, n))
        rhs = [[f[odd][yp, xp, here] for xp in (0, 1)] for yp in (0, 1)]
        scale = scale_rows(rhs[0][0].shape, z0 + 2 * at - LOW0 + odd, z_count)
        zs, old = NONE, NONE
        if fresh > 0:
            zs = [[v[1 - odd][yp, xp, below] + v[1 - odd][yp, xp, above] for xp in (0, 1)] for yp in (0, 1)]
        if fresh > 1:
            old = [[v[odd][yp, xp, here] for xp in (0, 1)] for yp in (0, 1)]
        new = phase0(old, rhs, zs, scale, steps)
        for yp, xp in YX:
            v[odd][yp, xp, here] = new[yp][xp]


def run1(v, f, z0, z_count, odd, low, high, steps, fresh):
    for at, n in chunks(low, high, CHUNK1):
        here = pl.ds(at, n)
        below, above = (pl.ds(at, n), pl.ds(at + 1, n)) if odd else (pl.ds(at - 1, n), pl.ds(at, n))
        g = [f[here, odd, yp] for yp in (0, 1)]
        scale = scale_rows(g[0].shape, z0 + 2 * at - LOW1 + odd, z_count)
        zs, old = NONE[0], NONE[0]
        if fresh > 0:
            zs = [v[1 - odd][yp, below] + v[1 - odd][yp, above] for yp in (0, 1)]
        if fresh > 1:
            old = [v[odd][yp, here] for yp in (0, 1)]
        new = phase1(old, g, zs, scale, steps)
        for yp in (0, 1):
            v[odd][yp, here] = new[yp]


def permutation(size, inverse):
    half = size // 2
    wide = lax.broadcasted_iota(jnp.int32, (size, size), 0 if inverse else 1)
    tall = lax.broadcasted_iota(jnp.int32, (size, size), 1 if inverse else 0)
    source = jnp.where(wide < half, 2 * wide, 2 * (wide - half) + 1)
    return jnp.where(tall == source, F32(1.0), F32(0.0))


def when(condition, act):
    @pl.when(condition)
    def _():
        act()


def send_order(far, halves):
    order = [(dz, h) for dz in (far, 0, -far) for h in reversed(range(halves))]
    return [(dz, h) for dz, h in order if dz != 0 or h != 0]


def receive_order(far, halves):
    order = [(dz, h) for h in range(halves) for dz in (0, -far, far)]
    return [(dz, h) for dz, h in order if dz != 0 or h != 0]


def kernel(
    gz_n, gy_n, rhs_hbm, sol_ref, res_ref, alpha_ref,
    flat, mine, got, fe, fo, ve, vo, dbuf, f1, v1e, v1o, vc, part, parts, nat,
    ssem, r1, r2, r3, rs, rhs_ref, s5, token,
):
    gz, gy = lax.axis_index("gz"), lax.axis_index("gy")
    zl, yl, nx = rhs_ref.shape
    fetch = pltpu.make_async_copy(rhs_hbm, rhs_ref, s5)
    fetch.start()
    y2, x2 = yl // 2, nx // 2
    yc = y2 // 2
    zc = zl // 2
    z_count = gz_n * zl
    z0 = gz * zl
    f, v = (fe, fo), (ve, vo)
    v1 = (v1e, v1o)
    halves = gy_n // 2
    sibling = gy + 1 - 2 * lax.rem(gy, 2)

    def there(dz):
        return (gz + dz >= 0) & (gz + dz < gz_n)

    def when_there(dz, go):
        if dz == 0:
            go()
        else:
            when(there(dz), go)

    barrier = pltpu.get_barrier_semaphore()
    count = jnp.int32(0)
    greet = [(dz, 2 * h) for h in reversed(range(halves)) for dz in (-1, 1)] + [(-2, 0), (2, 0)] + [(0, dg) for dg in range(1, gy_n)]
    for dz, dg in greet:

        def go(dz=dz, dg=dg):
            pl.semaphore_signal(
                barrier, inc=1, device_id=(gz + dz, lax.rem(gy + dg, gy_n)), device_id_type=MESH
            )

        when_there(dz, go)
        count = count + (1 if dz == 0 else there(dz).astype(jnp.int32))

    fetch.wait()
    lane = lax.broadcasted_iota(jnp.int32, (zl * yl, x2), 1)
    source = 2 * lax.rem(lane, x2 // 2)
    rows = rhs_ref[...].reshape(zl * yl, nx)
    for xp in (0, 1):
        left, right = (
            jnp.take_along_axis(rows[:, i : i + x2], source + xp, axis=1, mode="promise_in_bounds") for i in (0, x2)
        )
        flat[xp] = jnp.where(lane < x2 // 2, left, right)
    for z in range(zl):
        for yp, xp in YX:
            row = flat[xp, pl.ds(z * yl + yp, y2, stride=2), :]
            mine[z, (yp * 2 + xp) * y2 : (yp * 2 + xp + 1) * y2, :] = row
    got[gy, pl.ds(LOW0, zl)] = mine[...]

    @pl.when(gz == 0)
    def _():
        got[:, 0:LOW0] = jnp.zeros((gy_n, LOW0) + got.shape[2:], F32)

    @pl.when(gz == gz_n - 1)
    def _():
        got[:, LOW0 + zl :] = jnp.zeros((gy_n, WINDOW - LOW0 - zl) + got.shape[2:], F32)

    high = WINDOW - LOW0 - zl
    moves1 = {-1: (0, high, LOW0 + zl), 0: (0, zl, LOW0), 1: (zl - LOW0, LOW0, 0)}
    moves2 = {-2: (0, zc // 2, 7), -1: (0, zc // 2, 5), 1: (0, zc // 2, 1), 2: (zc // 2 - 1, 1, 0)}

    def pass_token(round_):
        reach = 2 << round_
        for dz in (-reach, reach):
            when_there(dz, lambda dz=dz: pl.semaphore_signal(
                token.at[round_], inc=1, device_id=(gz + dz, gy), device_id_type=MESH
            ))

    def take_token(round_):
        reach = 2 << round_
        pl.semaphore_wait(token.at[round_], there(-reach).astype(jnp.int32) + there(reach).astype(jnp.int32))

    def each_parity(index, act):
        for parity in (0, 1):
            when(lax.rem(index, 2) == parity, lambda parity=parity: act(parity))

    def unpack(dz, g):
        _, n, to = moves1[dz]
        for q in range(to, to + n):
            for k, (yp, xp) in enumerate(YX):
                f[q % 2][yp, xp, q // 2, g * y2 : (g + 1) * y2, :] = got[g, q, k * y2 : (k + 1) * y2, :]

    def gather():
        slots = {1: 0, -1: 1, 0: 2}

        def direct(dz, h, owner):
            first, n, to = moves1[dz]
            g = lax.rem(gy + 2 * h, gy_n)
            return pltpu.make_async_remote_copy(
                src_ref=mine.at[pl.ds(first, n)],
                dst_ref=got.at[g if owner else gy, pl.ds(to, n)],
                send_sem=ssem.at[slots[dz] * halves + h],
                recv_sem=r1.at[slots[dz], g if owner else gy],
                device_id=(gz - dz if owner else gz + dz, g),
                device_id_type=MESH,
            )

        def relay(dz, h, owner):
            _, n, to = moves1[dz]
            g = lax.rem((sibling if owner else gy) + 2 * h, gy_n)
            place = got.at[g, pl.ds(to, n)]
            return pltpu.make_async_remote_copy(
                src_ref=mine if dz == 0 and h == 0 else place,
                dst_ref=place,
                send_sem=ssem.at[(3 + slots[dz]) * halves + h],
                recv_sem=r1.at[slots[dz], g],
                device_id=(gz, sibling),
                device_id_type=MESH,
            )

        def sends(parity):
            far = -1 if parity == 0 else 1
            for dz, h in send_order(far, halves):
                when_there(dz, lambda: direct(dz, h, False).start())

        each_parity(gz, sends)
        relay(0, 0, False).start()

        def forwards(parity):
            far = 1 if parity == 0 else -1
            for dz, h in receive_order(far, halves):

                def go():
                    direct(dz, h, True).wait_recv()
                    relay(dz, h, False).start()

                when_there(-dz, go)

        each_parity(gz, forwards)
        if rounds > 0:
            pass_token(0)
        each_parity(gy, lambda parity: [unpack(dz, g) for dz in (0, 1, -1) for g in range(parity, gy_n, 2)])
        for dz in (0, 1, -1):
            for h in range(halves):
                when_there(-dz, lambda: relay(dz, h, True).wait_recv())
            each_parity(gy, lambda parity: [unpack(dz, g) for g in range(1 - parity, gy_n, 2)])
        for dz in (0, 1, -1):
            for h in range(halves):
                when_there(-dz, lambda: relay(dz, h, False).wait_send())
                if dz != 0 or h != 0:
                    when_there(dz, lambda: direct(dz, h, False).wait_send())

    rounds = max(gz_n - 2, 1).bit_length() - 1
    pl.semaphore_wait(barrier, count)
    gather()

    run0(v, f, z0, z_count, 0, 0, EVENS, PHASE_A, 0)
    run0(v, f, z0, z_count, 1, 0, ODDS, PHASE_B, 1)
    run0(v, f, z0, z_count, 0, 1, EVENS - 1, PHASE_C, 2)

    own = LOW0 // 2
    here, below, above = pl.ds(own, zc), pl.ds(own - 1, zc), pl.ds(own, zc)
    s = [[ve[yp, xp, here] + vo[yp, xp, below] + vo[yp, xp, above] for xp in (0, 1)] for yp in (0, 1)]
    tall = [s[0][xp] + pair_sum(s[1][xp], 0, 1) for xp in (0, 1)]
    dbuf[...] = fe[0, 0, here] - (27.0 * ve[0, 0, here] - (tall[0] + pair_sum(tall[1], 0, 2)))
    half = gy_n * yc
    for z in range(zc):
        for yp in (0, 1):
            f1[3 + z // 2, z % 2, yp] = dbuf[z, pl.ds(yp, half, stride=2), :]
    for edge, low, n in ((0, 0, 3), (1, 0, 1), (gz_n - 2, 7, 2), (gz_n - 1, 5, 4)):

        @pl.when(gz == edge)
        def _(low=low, n=n):
            f1[low : low + n] = jnp.zeros((n,) + f1.shape[1:], F32)

    sender = lax.rem(gy, 2) == 1
    slots2 = {dz: slot for slot, dz in enumerate((-1, 1, -2, 2))}

    def near(dz, target, mate):
        first, n, to = moves2[dz]
        return pltpu.make_async_remote_copy(
            src_ref=f1.at[pl.ds(3 + first, n)], dst_ref=f1.at[pl.ds(to, n)],
            send_sem=ssem.at[2 * slots2[dz] + mate], recv_sem=r2.at[slots2[dz]],
            device_id=(gz + dz, target), device_id_type=MESH,
        )

    def send_near(parity):
        far = -1 if parity == 0 else 1
        for dz in (far, 2 * far, -2 * far, -far):
            when_there(dz, lambda: [near(dz, g, mate).start() for mate, g in ((1, gy), (0, sibling))])

    if rounds > 0:
        take_token(0)
    if rounds > 1:
        pass_token(1)
    when(sender, lambda: each_parity(gz, send_near))
    for dz in moves2:
        when_there(-dz, lambda: near(dz, gy, 0).wait_recv())
    for dz in moves2:
        when(sender & there(dz), lambda: [near(dz, gy, mate).wait_send() for mate in (0, 1)])

    for r in range(1, rounds):
        take_token(r)
        if r + 1 < rounds:
            pass_token(r + 1)

    c0, c_count = gz * zc, gz_n * zc
    run1(v1, f1, c0, c_count, 0, 0, EVENS, PHASE_A, 0)
    run1(v1, f1, c0, c_count, 1, 0, ODDS, PHASE_B, 1)
    run1(v1, f1, c0, c_count, 0, 1, EVENS - 1, PHASE_C, 2)

    f2 = []
    for i in range(1, EVENS - 1):
        s = [v1e[yp, pl.ds(i, 1)] + v1o[yp, pl.ds(i - 1, 1)] + v1o[yp, pl.ds(i, 1)] for yp in (0, 1)]
        tall = s[0] + pair_sum(s[1], 0, 1)
        f2.append(f1[pl.ds(i, 1), 0, 0] - (27.0 * v1e[0, pl.ds(i, 1)] - (tall + both_sides(tall, 2, 1))))
    q0, q_count = gz * (zc // 2), gz_n * (zc // 2)
    f2e, f2o = f2[0::2], f2[1::2]
    scale2 = [scale_rows(f2[0].shape, q0 - LOW2 + i, q_count) for i in range(7)]
    even2 = [phase2(None, f2e[k], None, scale2[2 * k], PHASE_A) for k in range(4)]
    odd2 = [phase2(None, f2o[k], even2[k] + even2[k + 1], scale2[2 * k + 1], PHASE_B) for k in range(3)]
    for k in (1, 2):
        even2[k] = phase2(even2[k], f2e[k], odd2[k - 1] + odd2[k], scale2[2 * k], PHASE_C)
    v2 = [odd2[0], even2[1], odd2[1], even2[2], odd2[2]]
    in_lane = lax.broadcasted_iota(jnp.int32, v2[0].shape, 2) % 2 == 0
    for k in range(5):
        v1e[0, pl.ds(2 + k, 1)] = v1e[0, pl.ds(2 + k, 1)] + jnp.where(in_lane, v2[k], 0.0)

    run1(v1, f1, c0, c_count, 0, 2, 7, PHASE_A, 2)
    run1(v1, f1, c0, c_count, 1, 2, 6, PHASE_B, 2)
    run1(v1, f1, c0, c_count, 0, 3, 6, PHASE_C, 2)

    for c in range(-1, 6):
        odd = c % 2
        i = (c + LOW1 - odd) // 2
        for yp in (0, 1):
            vc[c + 1, pl.ds(yp, half, stride=2), :] = v1[odd][yp, i]
    ve[0, 0, pl.ds(1, 7)] = ve[0, 0, pl.ds(1, 7)] + vc[...]

    run0(v, f, z0, z_count, 0, 1, 8, PHASE_A, 2)
    run0(v, f, z0, z_count, 1, 1, 7, PHASE_B, 2)
    run0(v, f, z0, z_count, 0, 2, 7, PHASE_C, 2)

    numer = denom = None
    for odd in (0, 1):
        for k in range(zc):
            i = own + k
            here, below, above = pl.ds(i, 1), pl.ds(i - 1 + odd, 1), pl.ds(i + odd, 1)
            p = [[v[odd][yp, xp, here] for xp in (0, 1)] for yp in (0, 1)]
            s = [[p[yp][xp] + v[1 - odd][yp, xp, below] + v[1 - odd][yp, xp, above] for xp in (0, 1)] for yp in (0, 1)]
            b = box0(s)
            for yp, xp in YX:
                image = 27.0 * p[yp][xp] - b[yp][xp]
                numer = add(numer, f[odd][yp, xp, here] * p[yp][xp])
                denom = add(denom, p[yp][xp] * image)
                parity_at = k * 2 + odd
                nat[yp, xp, pl.ds(parity_at, 1)] = image
    rows = numer.shape[1]
    for j, total in enumerate((numer, denom)):
        acc = None
        for r in range(0, rows, 8):
            acc = add(acc, total[0, r : r + 8, :])
        part[pl.ds(j, 1), :] = jnp.sum(acc, axis=0, keepdims=True)

    def spread(d, target):
        return pltpu.make_async_remote_copy(
            src_ref=part, dst_ref=parts.at[gz], send_sem=rs, recv_sem=r3,
            device_id=(lax.rem(gz + d, gz_n), target), device_id_type=MESH,
        )

    @pl.when(sender)
    def _():
        for d in sorted(range(1, gz_n), key=lambda d: -min(d, gz_n - d) if gz_n > 8 else -d):
            for g in (sibling, gy):
                spread(d, g).start()

    parts[gz] = part[...]

    back = permutation(nx, True)
    for which, out in ((0, sol_ref), (1, res_ref)):
        for z in range(zl):
            for yp, xp in YX:
                if which == 0:
                    row = v[z % 2][yp, xp, own + z // 2, pl.ds(gy * y2, y2), :]
                else:
                    row = nat[yp, xp, z, pl.ds(gy * y2, y2), :]
                flat[xp, pl.ds(z * yl + yp, y2, stride=2), :] = row
        out[...] = jnp.dot(
            jnp.concatenate([flat[0], flat[1]], axis=1), back, precision=lax.Precision.HIGHEST, preferred_element_type=F32
        ).reshape(zl, yl, nx)

    others = parts.at[pl.ds(0, gz_n - 1)]
    pltpu.make_async_copy(others, others, r3).wait()
    when(sender, lambda: [pltpu.make_async_copy(others, others, rs).wait() for _ in range(2)])
    sums = parts[0]
    for d in range(1, gz_n):
        sums = sums + parts[d]
    alpha = jnp.sum(sums[0:1], axis=1, keepdims=True) / jnp.sum(sums[1:2], axis=1, keepdims=True)
    alpha_ref[...] = jnp.broadcast_to(alpha.reshape(1, 1), alpha_ref.shape)


def solution(mesh):
    gz_n, gy_n = mesh.shape["gz"], mesh.shape["gy"]

    def body(rhs):
        zl, yl, nx = rhs.shape
        y2, x2 = yl // 2, nx // 2
        y_half = gy_n * y2
        zc, yc = zl // 2, y2 // 2
        vmem = lambda *shape: pltpu.VMEM(shape, F32)
        dma = lambda *shape: pltpu.SemaphoreType.DMA(shape)
        p, image, alpha = pl.pallas_call(
            functools.partial(kernel, gz_n, gy_n),
            out_shape=[vmem(*rhs.shape)] * 2 + [vmem(yl, nx)],
            in_specs=[pl.BlockSpec(memory_space=pl.ANY)],
            out_specs=[pl.BlockSpec(memory_space=pltpu.VMEM)] * 3,
            scratch_shapes=[
                vmem(2, zl * yl, x2),
                vmem(zl, 4 * y2, x2),
                vmem(gy_n, WINDOW, 4 * y2, x2),
                vmem(2, 2, EVENS, y_half, x2),
                vmem(2, 2, ODDS, y_half, x2),
                vmem(2, 2, EVENS, y_half, x2),
                vmem(2, 2, ODDS, y_half, x2),
                vmem(zc, y_half, x2),
                vmem(9, 2, 2, gy_n * yc, x2),
                vmem(2, EVENS, gy_n * yc, x2),
                vmem(2, ODDS, gy_n * yc, x2),
                vmem(7, y_half, x2),
                vmem(2, x2),
                vmem(gz_n, 2, x2),
                vmem(2, 2, zl, y_half, x2),
                dma(max(6 * (gy_n // 2), 8)), dma(3, gy_n), dma(4), pltpu.SemaphoreType.DMA, pltpu.SemaphoreType.DMA,
                vmem(zl, yl, nx), pltpu.SemaphoreType.DMA,
                pltpu.SemaphoreType.REGULAR((max(1, max(gz_n - 2, 1).bit_length() - 1),)),
            ],
            compiler_params=pltpu.CompilerParams(has_side_effects=True, collective_id=0),
        )(rhs)
        return p * alpha, rhs - image * alpha

    return jax.shard_map(
        lambda rhs: tuple(body(rhs)),
        mesh=mesh,
        in_specs=(P("gz", "gy", None),),
        out_specs=(P("gz", "gy", None), P("gz", "gy", None)),
        check_vma=False,
    )
```

```python
import functools

import jax
import jax.numpy as jnp
from jax import lax
from jax.experimental import pallas as pl
from jax.experimental.pallas import tpu as pltpu
from jax.sharding import PartitionSpec as P

MESH = pl.DeviceIdType.MESH
F32 = jnp.float32

LOW0, LOW1, LOW2 = 4, 6, 2
EVENS, ODDS = 9, 8
WINDOW = EVENS + ODDS

PHASE_A = ((0, (0, 1)), (1, (0, 1)))
PHASE_B = ((0, (0, 1)), (1, (0, 1, 0)), (0, (1, 0)))
PHASE_C = ((1, (1, 0)), (0, (1, 0)))

CHUNK0 = 3
CHUNK1 = 9


def add(*terms):
    total = None
    for term in terms:
        if term is not None:
            total = term if total is None else total + term
    return total


def shift(x, axis, step):
    if x is None:
        return None
    size = x.shape[axis]
    moved = pltpu.roll(x, step % size, axis)
    index = lax.broadcasted_iota(jnp.int32, x.shape, axis)
    keep = index >= step if step > 0 else index < size + step
    return jnp.where(keep, moved, 0.0)


def pair_sum(other, parity, axis):
    return add(other, shift(other, axis, 1 if parity == 0 else -1))


def both_sides(x, axis, step):
    return add(shift(x, axis, step), shift(x, axis, -step))


def scale_rows(shape, first, count):
    row = first + 2 * lax.broadcasted_iota(jnp.int32, shape, 0)
    return jnp.where((row >= 0) & (row < count), F32(1.0 / 26.0), F32(0.0))


def box0(s):
    tall = [[add(s[yp][xp], pair_sum(s[1 - yp][xp], yp, 1)) for xp in (0, 1)] for yp in (0, 1)]
    return [[add(tall[yp][xp], pair_sum(tall[yp][1 - xp], xp, 2)) for xp in (0, 1)] for yp in (0, 1)]


def edge_some(x, axis, width, inner, outer, at_start, at_end):
    size = x.shape[axis]
    index = lax.broadcasted_iota(jnp.int32, x.shape, axis)
    edge = (index < width) if at_start else None
    if at_end:
        last = index >= size - width
        edge = last if edge is None else edge | last
    return x * jnp.where(edge, F32(outer), F32(inner))


def phase0(v, f, zs, scale, steps):
    v = [list(v[0]), list(v[1])]
    for yp, order in steps:
        w = [add(zs[yp][xp], pair_sum(add(zs[1 - yp][xp], v[1 - yp][xp]), yp, 1)) for xp in (0, 1)]
        a, b = order[0], order[1]
        near, far = (1, -1) if a == 0 else (-1, 1)
        u = add(w[b], v[yp][b])
        h = add(f[yp][a], w[a])
        q = add(w[a], h * scale)
        u_near = shift(u, 2, near)
        v[yp][a] = add(h, u, u_near) * scale
        twice = None if u is None else add(edge_some(u, 2, 1, 2.0, 1.0, a == 1, a == 0), u_near, shift(u, 2, far)) * scale
        q_far = shift(q, 2, far)
        if len(order) == 3:
            p = add(w[b], add(f[yp][b], w[b]) * scale)
            back = add(edge_some(q, 2, 1, 2.0, 1.0, a == 0, a == 1), q_far, shift(q, 2, near))
            thrice = add(edge_some(u, 2, 1, 3.0, 2.0, True, True), F32(3.0) * u_near, shift(u, 2, far), shift(u, 2, 2 * near))
            v[yp][a] = add(h, p, shift(p, 2, near), add(back, thrice * scale) * scale) * scale
        v[yp][b] = add(f[yp][b], w[b], q, q_far, twice) * scale
    return v


def box1(s):
    tall = [add(s[yp], pair_sum(s[1 - yp], yp, 1)) for yp in (0, 1)]
    return [add(t, both_sides(t, 2, 1)) for t in tall]


def line_pair(v, g, w, scale, parity, order, step):
    a, b = order[0], order[1]
    first = parity == a
    h = add(g, w)
    u = add(w, v)
    q = add(w, h * scale)
    if len(order) == 2:
        m = jnp.where(first, q, 0.0 if u is None else u)
        second = add(edge_some(m, 2, step, 2.0, 1.0, b == 0, b == 1), both_sides(m, 2, 2 * step))
        return add(h, both_sides(m, 2, step), second * jnp.where(first, F32(0.0), scale)) * scale
    m = jnp.where(first, q, u)
    second = add(edge_some(m, 2, step, 2.0, 1.0, True, True), both_sides(m, 2, 2 * step))
    here, there = (-step, step) if a == 0 else (step, -step)
    index = lax.broadcasted_iota(jnp.int32, scale.shape, 2)
    ends = (index < 2 * step) | (index >= scale.shape[2] - 2 * step)
    thrice = add(
        shift(u, 2, here) * jnp.where(ends, F32(2.0), F32(3.0)), F32(3.0) * shift(u, 2, there), both_sides(u, 2, 3 * step)
    )
    third = second + jnp.where(first, scale, F32(0.0)) * thrice
    return add(h, both_sides(q, 2, step), third * scale) * scale


def phase1(v, g, zs, scale, steps):
    v = list(v)
    parity = lax.broadcasted_iota(jnp.int32, scale.shape, 2) % 2
    for yp, order in steps:
        w = add(zs[yp], pair_sum(add(zs[1 - yp], v[1 - yp]), yp, 1))
        v[yp] = line_pair(v[yp], g[yp], w, scale, parity, order, 1)
    return v


def phase2(v, g, zs, scale, steps):
    shape = scale.shape
    y_par = lax.broadcasted_iota(jnp.int32, shape, 1) % 2
    x_par = (lax.broadcasted_iota(jnp.int32, shape, 2) // 2) % 2
    for yp, order in steps:
        w = add(zs, both_sides(add(zs, v), 1, 1))
        new = line_pair(v, g, w, scale, x_par, order, 2)
        v = jnp.where(y_par == yp, new, 0.0 if v is None else v)
    return v


def chunks(low, high, size):
    for start in range(low, high, size):
        yield start, min(size, high - start)


YX = [(0, 0), (0, 1), (1, 0), (1, 1)]


NONE = [[None, None], [None, None]]


def run0(v, f, z0, z_count, odd, low, high, steps, fresh):
    for at, n in chunks(low, high, CHUNK0):
        here = pl.ds(at, n)
        below, above = (pl.ds(at, n), pl.ds(at + 1, n)) if odd else (pl.ds(at - 1, n), pl.ds(at, n))
        rhs = [[f[odd][yp, xp, here] for xp in (0, 1)] for yp in (0, 1)]
        scale = scale_rows(rhs[0][0].shape, z0 + 2 * at - LOW0 + odd, z_count)
        zs, old = NONE, NONE
        if fresh > 0:
            zs = [[v[1 - odd][yp, xp, below] + v[1 - odd][yp, xp, above] for xp in (0, 1)] for yp in (0, 1)]
        if fresh > 1:
            old = [[v[odd][yp, xp, here] for xp in (0, 1)] for yp in (0, 1)]
        new = phase0(old, rhs, zs, scale, steps)
        for yp, xp in YX:
            v[odd][yp, xp, here] = new[yp][xp]


def run1(v, f, z0, z_count, odd, low, high, steps, fresh):
    for at, n in chunks(low, high, CHUNK1):
        here = pl.ds(at, n)
        below, above = (pl.ds(at, n), pl.ds(at + 1, n)) if odd else (pl.ds(at - 1, n), pl.ds(at, n))
        g = [f[odd, here, yp] for yp in (0, 1)]
        scale = scale_rows(g[0].shape, z0 + 2 * at - LOW1 + odd, z_count)
        zs, old = NONE[0], NONE[0]
        if fresh > 0:
            zs = [v[1 - odd][yp, below] + v[1 - odd][yp, above] for yp in (0, 1)]
        if fresh > 1:
            old = [v[odd][yp, here] for yp in (0, 1)]
        new = phase1(old, g, zs, scale, steps)
        for yp in (0, 1):
            v[odd][yp, here] = new[yp]


def permutation(size, inverse):
    half = size // 2
    wide = lax.broadcasted_iota(jnp.int32, (size, size), 0 if inverse else 1)
    tall = lax.broadcasted_iota(jnp.int32, (size, size), 1 if inverse else 0)
    source = jnp.where(wide < half, 2 * wide, 2 * (wide - half) + 1)
    return jnp.where(tall == source, F32(1.0), F32(0.0))


def when(condition, act):
    @pl.when(condition)
    def _():
        act()


def send_order(far, halves):
    order = [(dz, h) for dz in (far, 0, -far) for h in reversed(range(halves))]
    return [(dz, h) for dz, h in order if dz != 0 or h != 0]


def receive_order(far, halves):
    order = [(dz, h) for h in range(halves) for dz in (0, -far, far)]
    return [(dz, h) for dz, h in order if dz != 0 or h != 0]


def kernel(
    gz_n, gy_n, rhs_hbm, sol_ref, res_ref, alpha_ref,
    flat, mine, got, fe, fo, ve, vo, dbuf, f1, v1e, v1o, vc, part, parts, nat,
    ssem, r1, rr, s2, r2, r3, rs, rhs_ref, s5, token,
):
    gz, gy = lax.axis_index("gz"), lax.axis_index("gy")
    zl, yl, nx = rhs_ref.shape
    fetch = pltpu.make_async_copy(rhs_hbm, rhs_ref, s5)
    fetch.start()
    y2, x2 = yl // 2, nx // 2
    yc = y2 // 2
    zc = zl // 2
    z_count = gz_n * zl
    z0 = gz * zl
    f, v = (fe, fo), (ve, vo)
    v1 = (v1e, v1o)
    halves = gy_n // 2
    sibling = gy + 1 - 2 * lax.rem(gy, 2)

    def there(dz):
        return (gz + dz >= 0) & (gz + dz < gz_n)

    def when_there(dz, go):
        if dz == 0:
            go()
        else:
            when(there(dz), go)

    barrier = pltpu.get_barrier_semaphore()
    count = jnp.int32(0)
    greet = [(dz, 2 * h) for h in reversed(range(halves)) for dz in (-1, 1)] + [(-2, 0), (2, 0)] + [(0, dg) for dg in range(1, gy_n)]
    for dz, dg in greet:

        def go(dz=dz, dg=dg):
            pl.semaphore_signal(
                barrier, inc=1, device_id=(gz + dz, lax.rem(gy + dg, gy_n)), device_id_type=MESH
            )

        when_there(dz, go)
        count = count + (1 if dz == 0 else there(dz).astype(jnp.int32))

    fetch.wait()
    lane = lax.broadcasted_iota(jnp.int32, (zl * yl, x2), 1)
    source = 2 * lax.rem(lane, x2 // 2)
    rows = rhs_ref[...].reshape(zl * yl, nx)
    for xp in (0, 1):
        left, right = (
            jnp.take_along_axis(rows[:, i : i + x2], source + xp, axis=1, mode="promise_in_bounds") for i in (0, x2)
        )
        flat[xp] = jnp.where(lane < x2 // 2, left, right)
    for z in range(zl):
        for yp, xp in YX:
            row = flat[xp, pl.ds(z * yl + yp, y2, stride=2), :]
            mine[z % 2, z // 2, (yp * 2 + xp) * y2 : (yp * 2 + xp + 1) * y2, :] = row

    low = LOW0 // 2
    counts = (EVENS, ODDS)
    moves1 = [
        {1: (zc - low, low, 0), 0: (0, zc, low), -1: (0, counts[zp] - low - zc, low + zc)} for zp in (0, 1)
    ]
    moves2 = {-2: (0, zc // 2, 7), -1: (0, zc // 2, 5), 1: (0, zc // 2, 1), 2: (zc // 2 - 1, 1, 0)}

    def rows(zp, dz):
        _, n, to = moves1[zp][dz]
        return pl.ds(to + zp * EVENS, n)

    for zp in (0, 1):
        got[gy, rows(zp, 0)] = mine[zp]
        for dz, edge in ((1, 0), (-1, gz_n - 1)):

            @pl.when(gz == edge)
            def _(zp=zp, dz=dz):
                got[:, rows(zp, dz)] = jnp.zeros((gy_n, moves1[zp][dz][1]) + got.shape[2:], F32)

    def pass_token(round_):
        reach = 2 << round_
        for dz in (-reach, reach):
            when_there(dz, lambda dz=dz: pl.semaphore_signal(
                token.at[round_], inc=1, device_id=(gz + dz, gy), device_id_type=MESH
            ))

    def take_token(round_):
        reach = 2 << round_
        pl.semaphore_wait(token.at[round_], there(-reach).astype(jnp.int32) + there(reach).astype(jnp.int32))

    def each_parity(index, act):
        for parity in (0, 1):
            when(lax.rem(index, 2) == parity, lambda parity=parity: act(parity))

    def edges(act):
        when(gz == 0, lambda: act(0))
        when(gz == gz_n - 1, lambda: act(1))
        when((gz > 0) & (gz < gz_n - 1), lambda: act(None))

    def unpack(zp, dz, g):
        _, n, to = moves1[zp][dz]
        for i in range(to, to + n):
            for k, (yp, xp) in enumerate(YX):
                f[zp][yp, xp, i, g * y2 : (g + 1) * y2, :] = got[g, i + zp * EVENS, k * y2 : (k + 1) * y2, :]

    slots = {1: 0, -1: 1, 0: 2}

    def direct(zp, dz, h, owner):
        first, n, _ = moves1[zp][dz]
        g = lax.rem(gy + 2 * h, gy_n)
        source = g if owner else gy
        return pltpu.make_async_remote_copy(
            src_ref=mine.at[zp, pl.ds(first, n)],
            dst_ref=got.at[source, rows(zp, dz)],
            send_sem=ssem.at[0],
            recv_sem=r1.at[zp, slots[dz], lax.div(source, 2)],
            device_id=(gz - dz if owner else gz + dz, g),
            device_id_type=MESH,
        )

    def relay(zp, dz, h):
        place = got.at[lax.rem(gy + 2 * h, gy_n), rows(zp, dz)]
        return pltpu.make_async_remote_copy(
            src_ref=mine.at[zp] if dz == 0 and h == 0 else place,
            dst_ref=place,
            send_sem=ssem.at[1],
            recv_sem=rr.at[zp],
            device_id=(gz, sibling),
            device_id_type=MESH,
        )

    def wait_rows(sem, n):
        block = got.at[pl.ds(0, halves), pl.ds(0, n)]
        pltpu.make_async_copy(block, block, sem).wait()

    def gather():
        def sends(parity):
            far = -1 if parity == 0 else 1
            for zp in (0, 1):
                for dz, h in send_order(far, halves):
                    when_there(dz, lambda: direct(zp, dz, h, False).start())
                relay(zp, 0, 0).start()

        each_parity(gz, sends)

        def forwards(parity):
            far = 1 if parity == 0 else -1
            for zp in (0, 1):
                for dz, h in receive_order(far, halves):

                    def go():
                        direct(zp, dz, h, True).wait_recv()
                        relay(zp, dz, h).start()

                    when_there(-dz, go)

        each_parity(gz, forwards)
        if rounds > 0:
            pass_token(0)
        each_parity(gy, lambda parity: [
            unpack(zp, dz, g) for zp in (0, 1) for dz in (0, 1, -1) for g in range(parity, gy_n, 2)
        ])

    def relayed(zp):
        total = counts[zp]
        less = (moves1[zp][1][1], moves1[zp][-1][1])
        edges(lambda edge: wait_rows(rr.at[zp], total - (0 if edge is None else less[edge])))
        each_parity(gy, lambda parity: [unpack(zp, dz, g) for dz in (0, 1, -1) for g in range(1 - parity, gy_n, 2)])

    def sent():
        up, down = (sum(moves1[zp][dz][1] for zp in (0, 1)) for dz in (1, -1))
        own_rows = zl - zl // halves
        edges(lambda edge: wait_rows(ssem.at[0], own_rows + (down if edge != 0 else 0) + (up if edge != 1 else 0)))
        edges(lambda edge: wait_rows(ssem.at[1], zl + (up if edge != 0 else 0) + (down if edge != 1 else 0)))

    rounds = max(gz_n - 2, 1).bit_length() - 1
    pl.semaphore_wait(barrier, count)
    gather()

    relayed(0)
    run0(v, f, z0, z_count, 0, 0, EVENS, PHASE_A, 0)
    relayed(1)
    run0(v, f, z0, z_count, 1, 0, ODDS, PHASE_B, 1)
    run0(v, f, z0, z_count, 0, 1, EVENS - 1, PHASE_C, 2)

    own = LOW0 // 2
    here, below, above = pl.ds(own, zc), pl.ds(own - 1, zc), pl.ds(own, zc)
    s = [[ve[yp, xp, here] + vo[yp, xp, below] + vo[yp, xp, above] for xp in (0, 1)] for yp in (0, 1)]
    tall = [s[0][xp] + pair_sum(s[1][xp], 0, 1) for xp in (0, 1)]
    dbuf[...] = fe[0, 0, here] - (27.0 * ve[0, 0, here] - (tall[0] + pair_sum(tall[1], 0, 2)))
    half = gy_n * yc
    for z in range(zc):
        for yp in (0, 1):
            f1[z % 2, 3 + z // 2, yp] = dbuf[z, pl.ds(yp, half, stride=2), :]
    for edge, low, n in ((0, 0, 3), (1, 0, 1), (gz_n - 2, 7, 2), (gz_n - 1, 5, 4)):

        @pl.when(gz == edge)
        def _(low=low, n=n):
            f1[:, low : low + n] = jnp.zeros((2, n) + f1.shape[2:], F32)

    sender = lax.rem(gy, 2) == 1
    def near(zp, dz, target):
        first, n, to = moves2[dz]
        n = min(n, counts[zp] - to)
        return pltpu.make_async_remote_copy(
            src_ref=f1.at[zp, pl.ds(3 + first, n)], dst_ref=f1.at[zp, pl.ds(to, n)],
            send_sem=s2.at[zp], recv_sem=r2.at[zp],
            device_id=(gz + dz, target), device_id_type=MESH,
        )

    def send_near(parity):
        far = -1 if parity == 0 else 1
        for zp in (0, 1):
            for dz in (far, 2 * far, -2 * far, -far):
                when_there(dz, lambda: [near(zp, dz, g).start() for g in (gy, sibling)])

    def wait_near(sem, sign, zps, times):
        def take(missing):
            n = sum(min(moves2[dz][1], counts[zp] - moves2[dz][2]) for zp in zps for dz in moves2 if dz not in missing)
            block = f1.at[pl.ds(0, times), pl.ds(0, n)]
            pltpu.make_async_copy(block, block, sem).wait()

        low_side, high_side = (sign * 2, sign), (-sign * 2, -sign)
        when(gz == 0, lambda: take(low_side))
        when(gz == 1, lambda: take(low_side[:1]))
        when(gz == gz_n - 2, lambda: take(high_side[:1]))
        when(gz == gz_n - 1, lambda: take(high_side))
        when((gz > 1) & (gz < gz_n - 2), lambda: take(()))

    if rounds > 0:
        take_token(0)
    if rounds > 1:
        pass_token(1)
    when(sender, lambda: each_parity(gz, send_near))
    sent()
    c0, c_count = gz * zc, gz_n * zc
    wait_near(r2.at[0], 1, (0,), 1)
    run1(v1, f1, c0, c_count, 0, 0, EVENS, PHASE_A, 0)
    wait_near(r2.at[1], 1, (1,), 1)
    run1(v1, f1, c0, c_count, 1, 0, ODDS, PHASE_B, 1)
    run1(v1, f1, c0, c_count, 0, 1, EVENS - 1, PHASE_C, 2)

    f2 = []
    for i in range(1, EVENS - 1):
        s = [v1e[yp, pl.ds(i, 1)] + v1o[yp, pl.ds(i - 1, 1)] + v1o[yp, pl.ds(i, 1)] for yp in (0, 1)]
        tall = s[0] + pair_sum(s[1], 0, 1)
        f2.append(f1[0, pl.ds(i, 1), 0] - (27.0 * v1e[0, pl.ds(i, 1)] - (tall + both_sides(tall, 2, 1))))
    q0, q_count = gz * (zc // 2), gz_n * (zc // 2)
    f2e, f2o = f2[0::2], f2[1::2]
    scale2 = [scale_rows(f2[0].shape, q0 - LOW2 + i, q_count) for i in range(7)]
    even2 = [phase2(None, f2e[k], None, scale2[2 * k], PHASE_A) for k in range(4)]
    odd2 = [phase2(None, f2o[k], even2[k] + even2[k + 1], scale2[2 * k + 1], PHASE_B) for k in range(3)]
    for k in (1, 2):
        even2[k] = phase2(even2[k], f2e[k], odd2[k - 1] + odd2[k], scale2[2 * k], PHASE_C)
    v2 = [odd2[0], even2[1], odd2[1], even2[2], odd2[2]]
    in_lane = lax.broadcasted_iota(jnp.int32, v2[0].shape, 2) % 2 == 0
    for k in range(5):
        v1e[0, pl.ds(2 + k, 1)] = v1e[0, pl.ds(2 + k, 1)] + jnp.where(in_lane, v2[k], 0.0)

    run1(v1, f1, c0, c_count, 0, 2, 7, PHASE_A, 2)
    run1(v1, f1, c0, c_count, 1, 2, 6, PHASE_B, 2)
    run1(v1, f1, c0, c_count, 0, 3, 6, PHASE_C, 2)

    for c in range(-1, 6):
        odd = c % 2
        i = (c + LOW1 - odd) // 2
        for yp in (0, 1):
            vc[c + 1, pl.ds(yp, half, stride=2), :] = v1[odd][yp, i]
    ve[0, 0, pl.ds(1, 7)] = ve[0, 0, pl.ds(1, 7)] + vc[...]

    run0(v, f, z0, z_count, 0, 1, 8, PHASE_A, 2)
    run0(v, f, z0, z_count, 1, 1, 7, PHASE_B, 2)
    run0(v, f, z0, z_count, 0, 2, 7, PHASE_C, 2)

    numer = denom = None
    for odd in (0, 1):
        for k in range(zc):
            i = own + k
            here, below, above = pl.ds(i, 1), pl.ds(i - 1 + odd, 1), pl.ds(i + odd, 1)
            p = [[v[odd][yp, xp, here] for xp in (0, 1)] for yp in (0, 1)]
            s = [[p[yp][xp] + v[1 - odd][yp, xp, below] + v[1 - odd][yp, xp, above] for xp in (0, 1)] for yp in (0, 1)]
            b = box0(s)
            for yp, xp in YX:
                image = 27.0 * p[yp][xp] - b[yp][xp]
                numer = add(numer, f[odd][yp, xp, here] * p[yp][xp])
                denom = add(denom, p[yp][xp] * image)
                parity_at = k * 2 + odd
                nat[yp, xp, pl.ds(parity_at, 1)] = image
    rows = numer.shape[1]
    for j, total in enumerate((numer, denom)):
        acc = None
        for r in range(0, rows, 8):
            acc = add(acc, total[0, r : r + 8, :])
        part[pl.ds(j, 1), :] = jnp.sum(acc, axis=0, keepdims=True)

    for r in range(1, rounds):
        take_token(r)
        if r + 1 < rounds:
            pass_token(r + 1)

    def spread(d, target):
        return pltpu.make_async_remote_copy(
            src_ref=part, dst_ref=parts.at[gz], send_sem=rs, recv_sem=r3,
            device_id=(lax.rem(gz + d, gz_n), target), device_id_type=MESH,
        )

    @pl.when(sender)
    def _():
        for d in sorted(range(1, gz_n), key=lambda d: -min(d, gz_n - d) if gz_n > 8 else -d):
            for g in (sibling, gy):
                spread(d, g).start()

    parts[gz] = part[...]

    back = permutation(nx, True)
    for which, out in ((0, sol_ref), (1, res_ref)):
        for z in range(zl):
            for yp, xp in YX:
                if which == 0:
                    row = v[z % 2][yp, xp, own + z // 2, pl.ds(gy * y2, y2), :]
                else:
                    row = nat[yp, xp, z, pl.ds(gy * y2, y2), :]
                flat[xp, pl.ds(z * yl + yp, y2, stride=2), :] = row
        out[...] = jnp.dot(
            jnp.concatenate([flat[0], flat[1]], axis=1), back, precision=lax.Precision.HIGHEST, preferred_element_type=F32
        ).reshape(zl, yl, nx)

    others = parts.at[pl.ds(0, gz_n - 1)]
    pltpu.make_async_copy(others, others, r3).wait()
    when(sender, lambda: [wait_near(s2.at[zp], -1, (zp,), 2) for zp in (0, 1)])
    when(sender, lambda: [pltpu.make_async_copy(others, others, rs).wait() for _ in range(2)])
    sums = parts[0]
    for d in range(1, gz_n):
        sums = sums + parts[d]
    alpha = jnp.sum(sums[0:1], axis=1, keepdims=True) / jnp.sum(sums[1:2], axis=1, keepdims=True)
    alpha_ref[...] = jnp.broadcast_to(alpha.reshape(1, 1), alpha_ref.shape)


def solution(mesh):
    gz_n, gy_n = mesh.shape["gz"], mesh.shape["gy"]

    def body(rhs):
        zl, yl, nx = rhs.shape
        y2, x2 = yl // 2, nx // 2
        y_half = gy_n * y2
        zc, yc = zl // 2, y2 // 2
        vmem = lambda *shape: pltpu.VMEM(shape, F32)
        dma = lambda *shape: pltpu.SemaphoreType.DMA(shape)
        p, image, alpha = pl.pallas_call(
            functools.partial(kernel, gz_n, gy_n),
            out_shape=[vmem(*rhs.shape)] * 2 + [vmem(yl, nx)],
            in_specs=[pl.BlockSpec(memory_space=pl.ANY)],
            out_specs=[pl.BlockSpec(memory_space=pltpu.VMEM)] * 3,
            scratch_shapes=[
                vmem(2, zl * yl, x2),
                vmem(2, zc, 4 * y2, x2),
                vmem(gy_n, WINDOW, 4 * y2, x2),
                vmem(2, 2, EVENS, y_half, x2),
                vmem(2, 2, ODDS, y_half, x2),
                vmem(2, 2, EVENS, y_half, x2),
                vmem(2, 2, ODDS, y_half, x2),
                vmem(zc, y_half, x2),
                vmem(2, EVENS, 2, gy_n * yc, x2),
                vmem(2, EVENS, gy_n * yc, x2),
                vmem(2, ODDS, gy_n * yc, x2),
                vmem(7, y_half, x2),
                vmem(2, x2),
                vmem(gz_n, 2, x2),
                vmem(2, 2, zl, y_half, x2),
                dma(2), dma(2, 3, gy_n // 2), dma(2), dma(2), dma(2),
                pltpu.SemaphoreType.DMA, pltpu.SemaphoreType.DMA,
                vmem(zl, yl, nx), pltpu.SemaphoreType.DMA,
                pltpu.SemaphoreType.REGULAR((max(1, max(gz_n - 2, 1).bit_length() - 1),)),
            ],
            compiler_params=pltpu.CompilerParams(has_side_effects=True, collective_id=0),
        )(rhs)
        return p * alpha, rhs - image * alpha

    return jax.shard_map(
        lambda rhs: tuple(body(rhs)),
        mesh=mesh,
        in_specs=(P("gz", "gy", None),),
        out_specs=(P("gz", "gy", None), P("gz", "gy", None)),
        check_vma=False,
    )
```

```python
import functools

import jax
import jax.numpy as jnp
from jax import lax
from jax.experimental import pallas as pl
from jax.experimental.pallas import tpu as pltpu
from jax.sharding import PartitionSpec as P

MESH = pl.DeviceIdType.MESH
F32 = jnp.float32

LOW0, LOW1, LOW2 = 4, 6, 2
EVENS, ODDS = 9, 8
WINDOW = EVENS + ODDS

PHASE_A = ((0, (0, 1)), (1, (0, 1)))
PHASE_B = ((0, (0, 1)), (1, (0, 1, 0)), (0, (1, 0)))
PHASE_C = ((1, (1, 0)), (0, (1, 0)))

CHUNK0 = 3
CHUNK1 = 9


def add(*terms):
    total = None
    for term in terms:
        if term is not None:
            total = term if total is None else total + term
    return total


def shift(x, axis, step):
    if x is None:
        return None
    size = x.shape[axis]
    moved = pltpu.roll(x, step % size, axis)
    index = lax.broadcasted_iota(jnp.int32, x.shape, axis)
    keep = index >= step if step > 0 else index < size + step
    return jnp.where(keep, moved, 0.0)


def pair_sum(other, parity, axis):
    return add(other, shift(other, axis, 1 if parity == 0 else -1))


def both_sides(x, axis, step):
    return add(shift(x, axis, step), shift(x, axis, -step))


def scale_rows(shape, first, count):
    row = first + 2 * lax.broadcasted_iota(jnp.int32, shape, 0)
    return jnp.where((row >= 0) & (row < count), F32(1.0 / 26.0), F32(0.0))


def box0(s):
    tall = [[add(s[yp][xp], pair_sum(s[1 - yp][xp], yp, 1)) for xp in (0, 1)] for yp in (0, 1)]
    return [[add(tall[yp][xp], pair_sum(tall[yp][1 - xp], xp, 2)) for xp in (0, 1)] for yp in (0, 1)]


def edge_some(x, axis, width, inner, outer, at_start, at_end):
    size = x.shape[axis]
    index = lax.broadcasted_iota(jnp.int32, x.shape, axis)
    edge = (index < width) if at_start else None
    if at_end:
        last = index >= size - width
        edge = last if edge is None else edge | last
    return x * jnp.where(edge, F32(outer), F32(inner))


def phase0(v, f, zs, scale, steps):
    v = [list(v[0]), list(v[1])]
    for yp, order in steps:
        w = [add(zs[yp][xp], pair_sum(add(zs[1 - yp][xp], v[1 - yp][xp]), yp, 1)) for xp in (0, 1)]
        a, b = order[0], order[1]
        near, far = (1, -1) if a == 0 else (-1, 1)
        u = add(w[b], v[yp][b])
        h = add(f[yp][a], w[a])
        q = add(w[a], h * scale)
        u_near = shift(u, 2, near)
        v[yp][a] = add(h, u, u_near) * scale
        twice = None if u is None else add(edge_some(u, 2, 1, 2.0, 1.0, a == 1, a == 0), u_near, shift(u, 2, far)) * scale
        q_far = shift(q, 2, far)
        if len(order) == 3:
            p = add(w[b], add(f[yp][b], w[b]) * scale)
            back = add(edge_some(q, 2, 1, 2.0, 1.0, a == 0, a == 1), q_far, shift(q, 2, near))
            thrice = add(edge_some(u, 2, 1, 3.0, 2.0, True, True), F32(3.0) * u_near, shift(u, 2, far), shift(u, 2, 2 * near))
            v[yp][a] = add(h, p, shift(p, 2, near), add(back, thrice * scale) * scale) * scale
        v[yp][b] = add(f[yp][b], w[b], q, q_far, twice) * scale
    return v


def box1(s):
    tall = [add(s[yp], pair_sum(s[1 - yp], yp, 1)) for yp in (0, 1)]
    return [add(t, both_sides(t, 2, 1)) for t in tall]


def line_pair(v, g, w, scale, parity, order, step):
    a, b = order[0], order[1]
    first = parity == a
    h = add(g, w)
    u = add(w, v)
    q = add(w, h * scale)
    if len(order) == 2:
        m = jnp.where(first, q, 0.0 if u is None else u)
        second = add(edge_some(m, 2, step, 2.0, 1.0, b == 0, b == 1), both_sides(m, 2, 2 * step))
        return add(h, both_sides(m, 2, step), second * jnp.where(first, F32(0.0), scale)) * scale
    m = jnp.where(first, q, u)
    second = add(edge_some(m, 2, step, 2.0, 1.0, True, True), both_sides(m, 2, 2 * step))
    here, there = (-step, step) if a == 0 else (step, -step)
    index = lax.broadcasted_iota(jnp.int32, scale.shape, 2)
    ends = (index < 2 * step) | (index >= scale.shape[2] - 2 * step)
    thrice = add(
        shift(u, 2, here) * jnp.where(ends, F32(2.0), F32(3.0)), F32(3.0) * shift(u, 2, there), both_sides(u, 2, 3 * step)
    )
    third = second + jnp.where(first, scale, F32(0.0)) * thrice
    return add(h, both_sides(q, 2, step), third * scale) * scale


def phase1(v, g, zs, scale, steps):
    v = list(v)
    parity = lax.broadcasted_iota(jnp.int32, scale.shape, 2) % 2
    for yp, order in steps:
        w = add(zs[yp], pair_sum(add(zs[1 - yp], v[1 - yp]), yp, 1))
        v[yp] = line_pair(v[yp], g[yp], w, scale, parity, order, 1)
    return v


def phase2(v, g, zs, scale, steps):
    shape = scale.shape
    y_par = lax.broadcasted_iota(jnp.int32, shape, 1) % 2
    x_par = (lax.broadcasted_iota(jnp.int32, shape, 2) // 2) % 2
    for yp, order in steps:
        w = add(zs, both_sides(add(zs, v), 1, 1))
        new = line_pair(v, g, w, scale, x_par, order, 2)
        v = jnp.where(y_par == yp, new, 0.0 if v is None else v)
    return v


def chunks(low, high, size):
    for start in range(low, high, size):
        yield start, min(size, high - start)


YX = [(0, 0), (0, 1), (1, 0), (1, 1)]


NONE = [[None, None], [None, None]]


def run0(v, f, z0, z_count, odd, low, high, steps, fresh):
    for at, n in chunks(low, high, CHUNK0):
        here = pl.ds(at, n)
        below, above = (pl.ds(at, n), pl.ds(at + 1, n)) if odd else (pl.ds(at - 1, n), pl.ds(at, n))
        rhs = [[f[odd][yp, xp, here] for xp in (0, 1)] for yp in (0, 1)]
        scale = scale_rows(rhs[0][0].shape, z0 + 2 * at - LOW0 + odd, z_count)
        zs, old = NONE, NONE
        if fresh > 0:
            zs = [[v[1 - odd][yp, xp, below] + v[1 - odd][yp, xp, above] for xp in (0, 1)] for yp in (0, 1)]
        if fresh > 1:
            old = [[v[odd][yp, xp, here] for xp in (0, 1)] for yp in (0, 1)]
        new = phase0(old, rhs, zs, scale, steps)
        for yp, xp in YX:
            v[odd][yp, xp, here] = new[yp][xp]


def run1(v, f, z0, z_count, odd, low, high, steps, fresh):
    for at, n in chunks(low, high, CHUNK1):
        here = pl.ds(at, n)
        below, above = (pl.ds(at, n), pl.ds(at + 1, n)) if odd else (pl.ds(at - 1, n), pl.ds(at, n))
        g = [f[odd, here, yp] for yp in (0, 1)]
        scale = scale_rows(g[0].shape, z0 + 2 * at - LOW1 + odd, z_count)
        zs, old = NONE[0], NONE[0]
        if fresh > 0:
            zs = [v[1 - odd][yp, below] + v[1 - odd][yp, above] for yp in (0, 1)]
        if fresh > 1:
            old = [v[odd][yp, here] for yp in (0, 1)]
        new = phase1(old, g, zs, scale, steps)
        for yp in (0, 1):
            v[odd][yp, here] = new[yp]


def permutation(size, inverse):
    half = size // 2
    wide = lax.broadcasted_iota(jnp.int32, (size, size), 0 if inverse else 1)
    tall = lax.broadcasted_iota(jnp.int32, (size, size), 1 if inverse else 0)
    source = jnp.where(wide < half, 2 * wide, 2 * (wide - half) + 1)
    return jnp.where(tall == source, F32(1.0), F32(0.0))


def when(condition, act):
    @pl.when(condition)
    def _():
        act()


def send_order(far, halves):
    order = [(dz, h) for dz in (far, 0, -far) for h in reversed(range(halves))]
    return [(dz, h) for dz, h in order if dz != 0 or h != 0]


def receive_order(far, halves):
    order = [(dz, h) for h in range(halves) for dz in (0, -far, far)]
    return [(dz, h) for dz, h in order if dz != 0 or h != 0]


def kernel(
    gz_n, gy_n, rhs_hbm, sol_ref, res_ref, alpha_ref,
    flat, mine, plain, got, fe, fo, ve, vo, dbuf, f1, v1e, v1o, vc, part, parts, nat,
    ssem, r1, rr, s2, r2, r3, rs, rhs_ref, s5, token,
):
    gz, gy = lax.axis_index("gz"), lax.axis_index("gy")
    zl, yl, nx = rhs_ref.shape
    fetch = pltpu.make_async_copy(rhs_hbm, rhs_ref, s5)
    fetch.start()
    y2, x2 = yl // 2, nx // 2
    yc = y2 // 2
    zc = zl // 2
    z_count = gz_n * zl
    z0 = gz * zl
    f, v = (fe, fo), (ve, vo)
    v1 = (v1e, v1o)
    halves = gy_n // 2
    sibling = gy + 1 - 2 * lax.rem(gy, 2)

    def there(dz):
        return (gz + dz >= 0) & (gz + dz < gz_n)

    def when_there(dz, go):
        if dz == 0:
            go()
        else:
            when(there(dz), go)

    barrier = pltpu.get_barrier_semaphore()
    count = jnp.int32(0)
    greet = [(dz, 2 * h) for h in reversed(range(halves)) for dz in (-1, 1)] + [(-2, 0), (2, 0)] + [(0, dg) for dg in range(1, gy_n)]
    for dz, dg in greet:

        def go(dz=dz, dg=dg):
            pl.semaphore_signal(
                barrier, inc=1, device_id=(gz + dz, lax.rem(gy + dg, gy_n)), device_id_type=MESH
            )

        when_there(dz, go)
        count = count + (1 if dz == 0 else there(dz).astype(jnp.int32))

    fetch.wait()
    lane = lax.broadcasted_iota(jnp.int32, (zl * yl, x2), 1)
    source = 2 * lax.rem(lane, x2 // 2)
    rows = rhs_ref[...].reshape(zl * yl, nx)
    for xp in (0, 1):
        left, right = (
            jnp.take_along_axis(rows[:, i : i + x2], source + xp, axis=1, mode="promise_in_bounds") for i in (0, x2)
        )
        flat[xp] = jnp.where(lane < x2 // 2, left, right)
    for z in range(zl):
        for yp, xp in YX:
            row = flat[xp, pl.ds(z * yl + yp, y2, stride=2), :]
            mine[z % 2, z // 2, (yp * 2 + xp) * y2 : (yp * 2 + xp + 1) * y2, :] = row
            plain[z, (yp * 2 + xp) * y2 : (yp * 2 + xp + 1) * y2, :] = row

    parts1 = [
        {1: (zc - 1, (-2,)), 0: (0, tuple(range(0, zl, 2))), -1: (0, (zl,))},
        {1: (zc - 1, (-1,)), 0: (0, tuple(range(1, zl, 2)))},
        {1: (zl - LOW0, tuple(range(-LOW0, -2))), -1: (1, tuple(range(zl + 1, WINDOW - LOW0)))},
    ]
    place_of, at = {}, 0
    for part_ in parts1:
        for dz, (_, zs) in part_.items():
            for z in zs:
                place_of[z] = at
                at += 1
    messages = [(k, dz, h) for k, part_ in enumerate(parts1) for dz in part_ for h in range(halves) if dz or h]
    mail = {m: i for i, m in enumerate(messages)}
    moves2 = {-2: (0, zc // 2, 7), -1: (0, zc // 2, 5), 1: (0, zc // 2, 1), 2: (zc // 2 - 1, 1, 0)}
    counts = (EVENS, ODDS)

    def rows(k, dz):
        zs = parts1[k][dz][1]
        return pl.ds(place_of[zs[0]], len(zs))

    def outgoing(k, dz):
        first, zs = parts1[k][dz]
        return (plain if k == 2 else mine.at[k]).at[pl.ds(first, len(zs))]

    for k in (0, 1):
        got[gy, rows(k, 0)] = mine[k]
    for k, part_ in enumerate(parts1):
        for dz, edge in ((1, 0), (-1, gz_n - 1)):
            if dz in part_:

                @pl.when(gz == edge)
                def _(k=k, dz=dz):
                    got[:, rows(k, dz)] = jnp.zeros((gy_n, len(parts1[k][dz][1])) + got.shape[2:], F32)

    def pass_token(round_):
        reach = 2 << round_
        for dz in (-reach, reach):
            when_there(dz, lambda dz=dz: pl.semaphore_signal(
                token.at[round_], inc=1, device_id=(gz + dz, gy), device_id_type=MESH
            ))

    def take_token(round_):
        reach = 2 << round_
        pl.semaphore_wait(token.at[round_], there(-reach).astype(jnp.int32) + there(reach).astype(jnp.int32))

    def each_parity(index, act):
        for parity in (0, 1):
            when(lax.rem(index, 2) == parity, lambda parity=parity: act(parity))

    def edges(act):
        when(gz == 0, lambda: act(0))
        when(gz == gz_n - 1, lambda: act(1))
        when((gz > 0) & (gz < gz_n - 1), lambda: act(None))

    def unpack(k, g):
        for dz in parts1[k]:
            for z in parts1[k][dz][1]:
                for j, (yp, xp) in enumerate(YX):
                    row = got[g, place_of[z], j * y2 : (j + 1) * y2, :]
                    f[z % 2][yp, xp, (z + LOW0) // 2, g * y2 : (g + 1) * y2, :] = row

    def direct(k, dz, h, owner):
        g = lax.rem(gy + 2 * h, gy_n)
        return pltpu.make_async_remote_copy(
            src_ref=outgoing(k, dz),
            dst_ref=got.at[g if owner else gy, rows(k, dz)],
            send_sem=ssem.at[0],
            recv_sem=r1.at[mail[k, dz, (halves - h) % halves if owner else h]],
            device_id=(gz - dz if owner else gz + dz, g),
            device_id_type=MESH,
        )

    def relay(k, dz, h):
        place = got.at[lax.rem(gy + 2 * h, gy_n), rows(k, dz)]
        return pltpu.make_async_remote_copy(
            src_ref=mine.at[k] if dz == 0 and h == 0 else place,
            dst_ref=place,
            send_sem=ssem.at[1],
            recv_sem=rr.at[k],
            device_id=(gz, sibling),
            device_id_type=MESH,
        )

    def wait_rows(sem, n):
        block = got.at[pl.ds(0, halves), pl.ds(0, n)]
        pltpu.make_async_copy(block, block, sem).wait()

    def send(ks):
        def starts(parity):
            far = -1 if parity == 0 else 1
            for k in ks:
                for dz, h in send_order(far, halves):
                    if dz in parts1[k]:
                        when_there(dz, lambda: direct(k, dz, h, False).start())
                if 0 in parts1[k]:
                    relay(k, 0, 0).start()

        each_parity(gz, starts)

    def forward(ks):
        def forwards(parity):
            far = 1 if parity == 0 else -1
            for k in ks:
                for dz, h in receive_order(far, halves):

                    def go():
                        direct(k, dz, h, True).wait_recv()
                        relay(k, dz, h).start()

                    if dz in parts1[k]:
                        when_there(-dz, go)

        each_parity(gz, forwards)
        each_parity(gy, lambda parity: [unpack(k, g) for k in ks for g in range(parity, gy_n, 2)])

    def height(k, dz):
        return len(parts1[k][dz][1]) if dz in parts1[k] else 0

    def relayed(k):
        total = sum(height(k, dz) for dz in (-1, 0, 1))
        less = (height(k, 1), height(k, -1))
        edges(lambda edge: wait_rows(rr.at[k], total - (0 if edge is None else less[edge])))
        each_parity(gy, lambda parity: [unpack(k, g) for g in range(1 - parity, gy_n, 2)])

    def sent():
        up, down = (sum(height(k, dz) for k in range(3)) for dz in (1, -1))
        own_rows = zl - zl // halves
        edges(lambda edge: wait_rows(ssem.at[0], own_rows + (down if edge != 0 else 0) + (up if edge != 1 else 0)))
        edges(lambda edge: wait_rows(ssem.at[1], zl + (up if edge != 0 else 0) + (down if edge != 1 else 0)))

    rounds = max(gz_n - 2, 1).bit_length() - 1
    pl.semaphore_wait(barrier, count)
    own = LOW0 // 2
    last = own + zc
    send((0, 1, 2))
    forward((0, 1))
    if rounds > 0:
        pass_token(0)
    relayed(0)
    run0(v, f, z0, z_count, 0, own - 1, last + 1, PHASE_A, 0)
    relayed(1)
    run0(v, f, z0, z_count, 1, own - 1, last, PHASE_B, 1)
    run0(v, f, z0, z_count, 0, own, last, PHASE_C, 2)

    here, below, above = pl.ds(own, zc), pl.ds(own - 1, zc), pl.ds(own, zc)
    s = [[ve[yp, xp, here] + vo[yp, xp, below] + vo[yp, xp, above] for xp in (0, 1)] for yp in (0, 1)]
    tall = [s[0][xp] + pair_sum(s[1][xp], 0, 1) for xp in (0, 1)]
    dbuf[...] = fe[0, 0, here] - (27.0 * ve[0, 0, here] - (tall[0] + pair_sum(tall[1], 0, 2)))
    half = gy_n * yc
    for z in range(zc):
        for yp in (0, 1):
            f1[z % 2, 3 + z // 2, yp] = dbuf[z, pl.ds(yp, half, stride=2), :]
    for edge, low, n in ((0, 0, 3), (1, 0, 1), (gz_n - 2, 7, 2), (gz_n - 1, 5, 4)):

        @pl.when(gz == edge)
        def _(low=low, n=n):
            f1[:, low : low + n] = jnp.zeros((2, n) + f1.shape[2:], F32)

    sender = lax.rem(gy, 2) == 1
    def near(zp, dz, target):
        first, n, to = moves2[dz]
        n = min(n, counts[zp] - to)
        return pltpu.make_async_remote_copy(
            src_ref=f1.at[zp, pl.ds(3 + first, n)], dst_ref=f1.at[zp, pl.ds(to, n)],
            send_sem=s2.at[zp], recv_sem=r2.at[zp],
            device_id=(gz + dz, target), device_id_type=MESH,
        )

    def send_near(parity):
        far = -1 if parity == 0 else 1
        for zp in (0, 1):
            for dz in (far, 2 * far, -2 * far, -far):
                when_there(dz, lambda: [near(zp, dz, g).start() for g in (gy, sibling)])

    def wait_near(sem, sign, zps, times):
        def take(missing):
            n = sum(min(moves2[dz][1], counts[zp] - moves2[dz][2]) for zp in zps for dz in moves2 if dz not in missing)
            block = f1.at[pl.ds(0, times), pl.ds(0, n)]
            pltpu.make_async_copy(block, block, sem).wait()

        low_side, high_side = (sign * 2, sign), (-sign * 2, -sign)
        when(gz == 0, lambda: take(low_side))
        when(gz == 1, lambda: take(low_side[:1]))
        when(gz == gz_n - 2, lambda: take(high_side[:1]))
        when(gz == gz_n - 1, lambda: take(high_side))
        when((gz > 1) & (gz < gz_n - 2), lambda: take(()))

    if rounds > 0:
        take_token(0)
    if rounds > 1:
        pass_token(1)
    when(sender, lambda: each_parity(gz, send_near))
    forward((2,))
    relayed(2)
    for phase, odd, ranges in (
        (PHASE_A, 0, ((0, own - 1), (last + 1, EVENS))),
        (PHASE_B, 1, ((0, own - 1), (last, ODDS))),
        (PHASE_C, 0, ((1, own), (last, EVENS - 1))),
    ):
        for low, high in ranges:
            run0(v, f, z0, z_count, odd, low, high, phase, odd if phase is not PHASE_C else 2)
    sent()
    c0, c_count = gz * zc, gz_n * zc
    wait_near(r2.at[0], 1, (0,), 1)
    run1(v1, f1, c0, c_count, 0, 0, EVENS, PHASE_A, 0)
    wait_near(r2.at[1], 1, (1,), 1)
    run1(v1, f1, c0, c_count, 1, 0, ODDS, PHASE_B, 1)
    run1(v1, f1, c0, c_count, 0, 1, EVENS - 1, PHASE_C, 2)

    f2 = []
    for i in range(1, EVENS - 1):
        s = [v1e[yp, pl.ds(i, 1)] + v1o[yp, pl.ds(i - 1, 1)] + v1o[yp, pl.ds(i, 1)] for yp in (0, 1)]
        tall = s[0] + pair_sum(s[1], 0, 1)
        f2.append(f1[0, pl.ds(i, 1), 0] - (27.0 * v1e[0, pl.ds(i, 1)] - (tall + both_sides(tall, 2, 1))))
    q0, q_count = gz * (zc // 2), gz_n * (zc // 2)
    f2e, f2o = f2[0::2], f2[1::2]
    scale2 = [scale_rows(f2[0].shape, q0 - LOW2 + i, q_count) for i in range(7)]
    even2 = [phase2(None, f2e[k], None, scale2[2 * k], PHASE_A) for k in range(4)]
    odd2 = [phase2(None, f2o[k], even2[k] + even2[k + 1], scale2[2 * k + 1], PHASE_B) for k in range(3)]
    for k in (1, 2):
        even2[k] = phase2(even2[k], f2e[k], odd2[k - 1] + odd2[k], scale2[2 * k], PHASE_C)
    v2 = [odd2[0], even2[1], odd2[1], even2[2], odd2[2]]
    in_lane = lax.broadcasted_iota(jnp.int32, v2[0].shape, 2) % 2 == 0
    for k in range(5):
        v1e[0, pl.ds(2 + k, 1)] = v1e[0, pl.ds(2 + k, 1)] + jnp.where(in_lane, v2[k], 0.0)

    run1(v1, f1, c0, c_count, 0, 2, 7, PHASE_A, 2)
    run1(v1, f1, c0, c_count, 1, 2, 6, PHASE_B, 2)
    run1(v1, f1, c0, c_count, 0, 3, 6, PHASE_C, 2)

    for c in range(-1, 6):
        odd = c % 2
        i = (c + LOW1 - odd) // 2
        for yp in (0, 1):
            vc[c + 1, pl.ds(yp, half, stride=2), :] = v1[odd][yp, i]
    ve[0, 0, pl.ds(1, 7)] = ve[0, 0, pl.ds(1, 7)] + vc[...]

    run0(v, f, z0, z_count, 0, 1, 8, PHASE_A, 2)
    run0(v, f, z0, z_count, 1, 1, 7, PHASE_B, 2)
    run0(v, f, z0, z_count, 0, 2, 7, PHASE_C, 2)

    numer = denom = None
    for odd in (0, 1):
        for k in range(zc):
            i = own + k
            here, below, above = pl.ds(i, 1), pl.ds(i - 1 + odd, 1), pl.ds(i + odd, 1)
            p = [[v[odd][yp, xp, here] for xp in (0, 1)] for yp in (0, 1)]
            s = [[p[yp][xp] + v[1 - odd][yp, xp, below] + v[1 - odd][yp, xp, above] for xp in (0, 1)] for yp in (0, 1)]
            b = box0(s)
            for yp, xp in YX:
                image = 27.0 * p[yp][xp] - b[yp][xp]
                numer = add(numer, f[odd][yp, xp, here] * p[yp][xp])
                denom = add(denom, p[yp][xp] * image)
                parity_at = k * 2 + odd
                nat[yp, xp, pl.ds(parity_at, 1)] = image
    rows = numer.shape[1]
    for j, total in enumerate((numer, denom)):
        acc = None
        for r in range(0, rows, 8):
            acc = add(acc, total[0, r : r + 8, :])
        part[pl.ds(j, 1), :] = jnp.sum(acc, axis=0, keepdims=True)

    for r in range(1, rounds):
        take_token(r)
        if r + 1 < rounds:
            pass_token(r + 1)

    def spread(to, target):
        return pltpu.make_async_remote_copy(
            src_ref=part, dst_ref=parts.at[gz], send_sem=rs, recv_sem=r3,
            device_id=(to, target), device_id_type=MESH,
        )

    @pl.when(sender)
    def _():
        for to in range(gz_n):

            def go():
                for g in (sibling, gy):
                    spread(to, g).start()

            when(gz != to, go)

    parts[gz] = part[...]

    back = permutation(nx, True)
    for which, out in ((0, sol_ref), (1, res_ref)):
        for z in range(zl):
            for yp, xp in YX:
                if which == 0:
                    row = v[z % 2][yp, xp, own + z // 2, pl.ds(gy * y2, y2), :]
                else:
                    row = nat[yp, xp, z, pl.ds(gy * y2, y2), :]
                flat[xp, pl.ds(z * yl + yp, y2, stride=2), :] = row
        out[...] = jnp.dot(
            jnp.concatenate([flat[0], flat[1]], axis=1), back, precision=lax.Precision.HIGHEST, preferred_element_type=F32
        ).reshape(zl, yl, nx)

    others = parts.at[pl.ds(0, gz_n - 1)]
    pltpu.make_async_copy(others, others, r3).wait()
    when(sender, lambda: [wait_near(s2.at[zp], -1, (zp,), 2) for zp in (0, 1)])
    when(sender, lambda: [pltpu.make_async_copy(others, others, rs).wait() for _ in range(2)])
    sums = parts[0]
    for d in range(1, gz_n):
        sums = sums + parts[d]
    alpha = jnp.sum(sums[0:1], axis=1, keepdims=True) / jnp.sum(sums[1:2], axis=1, keepdims=True)
    alpha_ref[...] = jnp.broadcast_to(alpha.reshape(1, 1), alpha_ref.shape)


def solution(mesh):
    gz_n, gy_n = mesh.shape["gz"], mesh.shape["gy"]

    def body(rhs):
        zl, yl, nx = rhs.shape
        y2, x2 = yl // 2, nx // 2
        y_half = gy_n * y2
        zc, yc = zl // 2, y2 // 2
        vmem = lambda *shape: pltpu.VMEM(shape, F32)
        dma = lambda *shape: pltpu.SemaphoreType.DMA(shape)
        p, image, alpha = pl.pallas_call(
            functools.partial(kernel, gz_n, gy_n),
            out_shape=[vmem(*rhs.shape)] * 2 + [vmem(yl, nx)],
            in_specs=[pl.BlockSpec(memory_space=pl.ANY)],
            out_specs=[pl.BlockSpec(memory_space=pltpu.VMEM)] * 3,
            scratch_shapes=[
                vmem(2, zl * yl, x2),
                vmem(2, zc, 4 * y2, x2),
                vmem(zl, 4 * y2, x2),
                vmem(gy_n, WINDOW, 4 * y2, x2),
                vmem(2, 2, EVENS, y_half, x2),
                vmem(2, 2, ODDS, y_half, x2),
                vmem(2, 2, EVENS, y_half, x2),
                vmem(2, 2, ODDS, y_half, x2),
                vmem(zc, y_half, x2),
                vmem(2, EVENS, 2, gy_n * yc, x2),
                vmem(2, EVENS, gy_n * yc, x2),
                vmem(2, ODDS, gy_n * yc, x2),
                vmem(7, y_half, x2),
                vmem(2, x2),
                vmem(gz_n, 2, x2),
                vmem(2, 2, zl, y_half, x2),
                dma(2), dma(7 * (gy_n // 2) - 2), dma(3), dma(2), dma(2),
                pltpu.SemaphoreType.DMA, pltpu.SemaphoreType.DMA,
                vmem(zl, yl, nx), pltpu.SemaphoreType.DMA,
                pltpu.SemaphoreType.REGULAR((max(1, max(gz_n - 2, 1).bit_length() - 1),)),
            ],
            compiler_params=pltpu.CompilerParams(has_side_effects=True, collective_id=0),
        )(rhs)
        return p * alpha, rhs - image * alpha

    return jax.shard_map(
        lambda rhs: tuple(body(rhs)),
        mesh=mesh,
        in_specs=(P("gz", "gy", None),),
        out_specs=(P("gz", "gy", None), P("gz", "gy", None)),
        check_vma=False,
    )
```

```python
import functools

import jax
import jax.numpy as jnp
from jax import lax
from jax.experimental import pallas as pl
from jax.experimental.pallas import tpu as pltpu
from jax.sharding import PartitionSpec as P

MESH = pl.DeviceIdType.MESH
F32 = jnp.float32

LOW0, LOW1, LOW2 = 4, 6, 2
EVENS, ODDS = 9, 8
WINDOW = EVENS + ODDS

PHASE_A = ((0, (0, 1)), (1, (0, 1)))
PHASE_B = ((0, (0, 1)), (1, (0, 1, 0)), (0, (1, 0)))
PHASE_C = ((1, (1, 0)), (0, (1, 0)))

CHUNK0 = 3
CHUNK1 = 9


def add(*terms):
    total = None
    for term in terms:
        if term is not None:
            total = term if total is None else total + term
    return total


def shift(x, axis, step):
    if x is None:
        return None
    size = x.shape[axis]
    moved = pltpu.roll(x, step % size, axis)
    index = lax.broadcasted_iota(jnp.int32, x.shape, axis)
    keep = index >= step if step > 0 else index < size + step
    return jnp.where(keep, moved, 0.0)


def pair_sum(other, parity, axis):
    return add(other, shift(other, axis, 1 if parity == 0 else -1))


def both_sides(x, axis, step):
    return add(shift(x, axis, step), shift(x, axis, -step))


def scale_rows(shape, first, count):
    row = first + 2 * lax.broadcasted_iota(jnp.int32, shape, 0)
    return jnp.where((row >= 0) & (row < count), F32(1.0 / 26.0), F32(0.0))


def box0(s):
    tall = [[add(s[yp][xp], pair_sum(s[1 - yp][xp], yp, 1)) for xp in (0, 1)] for yp in (0, 1)]
    return [[add(tall[yp][xp], pair_sum(tall[yp][1 - xp], xp, 2)) for xp in (0, 1)] for yp in (0, 1)]


def edge_some(x, axis, width, inner, outer, at_start, at_end):
    size = x.shape[axis]
    index = lax.broadcasted_iota(jnp.int32, x.shape, axis)
    edge = (index < width) if at_start else None
    if at_end:
        last = index >= size - width
        edge = last if edge is None else edge | last
    return x * jnp.where(edge, F32(outer), F32(inner))


def phase0(v, f, zs, scale, steps):
    v = [list(v[0]), list(v[1])]
    for yp, order in steps:
        w = [add(zs[yp][xp], pair_sum(add(zs[1 - yp][xp], v[1 - yp][xp]), yp, 1)) for xp in (0, 1)]
        a, b = order[0], order[1]
        near, far = (1, -1) if a == 0 else (-1, 1)
        u = add(w[b], v[yp][b])
        h = add(f[yp][a], w[a])
        q = add(w[a], h * scale)
        y_far = shift(q if u is None else q + u * scale, 2, far)
        if u is None:
            v[yp][a] = h * scale
            v[yp][b] = add(f[yp][b], w[b], q, y_far) * scale
            continue
        u_near = shift(u, 2, near)
        if len(order) == 3:
            p = add(w[b], add(f[yp][b], w[b]) * scale)
            x_near = shift(p + scale * (q + F32(3.0) * (scale * u)), 2, near)
            thrice = edge_some(u, 2, 1, 3.0, 2.0, True, True) + shift(u, 2, 2 * near)
            inner = edge_some(q, 2, 1, 2.0, 1.0, a == 0, a == 1) + y_far + scale * thrice
            v[yp][a] = add(h, p, x_near, scale * inner) * scale
        else:
            v[yp][a] = add(h, u, u_near) * scale
        twice = edge_some(u, 2, 1, 2.0, 1.0, a == 1, a == 0) + u_near
        v[yp][b] = add(f[yp][b], w[b], q, y_far, twice * scale) * scale
    return v


def box1(s):
    tall = [add(s[yp], pair_sum(s[1 - yp], yp, 1)) for yp in (0, 1)]
    return [add(t, both_sides(t, 2, 1)) for t in tall]


def line_pair(v, g, w, scale, parity, order, step):
    a, b = order[0], order[1]
    first = parity == a
    h = add(g, w)
    u = add(w, v)
    q = add(w, h * scale)
    if u is None:
        return add(h, both_sides(jnp.where(first, q, 0.0), 2, step)) * scale
    m = jnp.where(first, q, u)
    second = add(edge_some(m, 2, step, 2.0, 1.0, True, True), both_sides(m, 2, 2 * step)) * scale
    if len(order) == 2:
        return add(h, both_sides(m, 2, step), jnp.where(first, 0.0, second)) * scale
    here, there = (-step, step) if a == 0 else (step, -step)
    index = lax.broadcasted_iota(jnp.int32, scale.shape, 2)
    ends = (index < 2 * step) | (index >= scale.shape[2] - 2 * step)
    square = scale * scale
    some = square * u
    m_here = jnp.where(first, q, q + some * jnp.where(ends, F32(2.0), F32(3.0)))
    m_there = jnp.where(first, q, q + some * F32(3.0))
    third = jnp.where(first, square * both_sides(u, 2, 3 * step), 0.0)
    return add(h, shift(m_here, 2, here), shift(m_there, 2, there), second, third) * scale


def phase1(v, g, zs, scale, steps):
    v = list(v)
    parity = lax.broadcasted_iota(jnp.int32, scale.shape, 2) % 2
    for yp, order in steps:
        w = add(zs[yp], pair_sum(add(zs[1 - yp], v[1 - yp]), yp, 1))
        v[yp] = line_pair(v[yp], g[yp], w, scale, parity, order, 1)
    return v


def phase2(v, g, zs, scale, steps):
    shape = scale.shape
    y_par = lax.broadcasted_iota(jnp.int32, shape, 1) % 2
    x_par = (lax.broadcasted_iota(jnp.int32, shape, 2) // 2) % 2
    for yp, order in steps:
        w = add(zs, both_sides(add(zs, v), 1, 1))
        new = line_pair(v, g, w, scale, x_par, order, 2)
        v = jnp.where(y_par == yp, new, 0.0 if v is None else v)
    return v


def chunks(low, high, size):
    for start in range(low, high, size):
        yield start, min(size, high - start)


YX = [(0, 0), (0, 1), (1, 0), (1, 1)]


NONE = [[None, None], [None, None]]


def run0(v, f, z0, z_count, odd, low, high, steps, fresh):
    for at, n in chunks(low, high, CHUNK0):
        here = pl.ds(at, n)
        below, above = (pl.ds(at, n), pl.ds(at + 1, n)) if odd else (pl.ds(at - 1, n), pl.ds(at, n))
        rhs = [[f[odd][yp, xp, here] for xp in (0, 1)] for yp in (0, 1)]
        scale = scale_rows(rhs[0][0].shape, z0 + 2 * at - LOW0 + odd, z_count)
        zs, old = NONE, NONE
        if fresh > 0:
            zs = [[v[1 - odd][yp, xp, below] + v[1 - odd][yp, xp, above] for xp in (0, 1)] for yp in (0, 1)]
        if fresh > 1:
            old = [[v[odd][yp, xp, here] for xp in (0, 1)] for yp in (0, 1)]
        new = phase0(old, rhs, zs, scale, steps)
        for yp, xp in YX:
            v[odd][yp, xp, here] = new[yp][xp]


def run1(v, f, z0, z_count, odd, low, high, steps, fresh):
    for at, n in chunks(low, high, CHUNK1):
        here = pl.ds(at, n)
        below, above = (pl.ds(at, n), pl.ds(at + 1, n)) if odd else (pl.ds(at - 1, n), pl.ds(at, n))
        g = [f[odd, here, yp] for yp in (0, 1)]
        scale = scale_rows(g[0].shape, z0 + 2 * at - LOW1 + odd, z_count)
        zs, old = NONE[0], NONE[0]
        if fresh > 0:
            zs = [v[1 - odd][yp, below] + v[1 - odd][yp, above] for yp in (0, 1)]
        if fresh > 1:
            old = [v[odd][yp, here] for yp in (0, 1)]
        new = phase1(old, g, zs, scale, steps)
        for yp in (0, 1):
            v[odd][yp, here] = new[yp]


def permutation(size, inverse):
    half = size // 2
    wide = lax.broadcasted_iota(jnp.int32, (size, size), 0 if inverse else 1)
    tall = lax.broadcasted_iota(jnp.int32, (size, size), 1 if inverse else 0)
    source = jnp.where(wide < half, 2 * wide, 2 * (wide - half) + 1)
    return jnp.where(tall == source, F32(1.0), F32(0.0))


def when(condition, act):
    @pl.when(condition)
    def _():
        act()


def send_order(far, halves):
    order = [(dz, h) for dz in (0, far, -far) for h in reversed(range(halves))]
    return [(dz, h) for dz, h in order if dz != 0 or h != 0]


def receive_order(far, halves):
    order = [(dz, h) for h in range(halves) for dz in (0, -far, far)]
    return [(dz, h) for dz, h in order if dz != 0 or h != 0]


def kernel(
    gz_n, gy_n, rhs_hbm, sol_ref, res_ref, alpha_ref,
    flat, mine, plain, got, fe, fo, ve, vo, dbuf, f1, v1e, v1o, vc, part, parts, nat,
    ssem, r1, rr, s2, r2, r3, rs, rhs_ref, s5, token,
):
    gz, gy = lax.axis_index("gz"), lax.axis_index("gy")
    zl, yl, nx = rhs_ref.shape
    fetch = pltpu.make_async_copy(rhs_hbm, rhs_ref, s5)
    fetch.start()
    y2, x2 = yl // 2, nx // 2
    yc = y2 // 2
    zc = zl // 2
    z_count = gz_n * zl
    z0 = gz * zl
    f, v = (fe, fo), (ve, vo)
    v1 = (v1e, v1o)
    halves = gy_n // 2
    sibling = gy + 1 - 2 * lax.rem(gy, 2)

    def there(dz):
        return (gz + dz >= 0) & (gz + dz < gz_n)

    def when_there(dz, go):
        if dz == 0:
            go()
        else:
            when(there(dz), go)

    barrier = pltpu.get_barrier_semaphore()
    count = jnp.int32(0)
    greet = [(dz, 2 * h) for h in reversed(range(halves)) for dz in (-1, 1)] + [(-2, 0), (2, 0)] + [(0, dg) for dg in range(1, gy_n)]
    for dz, dg in greet:

        def go(dz=dz, dg=dg):
            pl.semaphore_signal(
                barrier, inc=1, device_id=(gz + dz, lax.rem(gy + dg, gy_n)), device_id_type=MESH
            )

        when_there(dz, go)
        count = count + (1 if dz == 0 else there(dz).astype(jnp.int32))

    fetch.wait()
    lane = lax.broadcasted_iota(jnp.int32, (zl * yl, x2), 1)
    source = 2 * lax.rem(lane, x2 // 2)
    rows = rhs_ref[...].reshape(zl * yl, nx)
    for xp in (0, 1):
        left, right = (
            jnp.take_along_axis(rows[:, i : i + x2], source + xp, axis=1, mode="promise_in_bounds") for i in (0, x2)
        )
        flat[xp] = jnp.where(lane < x2 // 2, left, right)
    for z in range(zl):
        for yp, xp in YX:
            row = flat[xp, pl.ds(z * yl + yp, y2, stride=2), :]
            mine[z % 2, z // 2, (yp * 2 + xp) * y2 : (yp * 2 + xp + 1) * y2, :] = row
            plain[z, (yp * 2 + xp) * y2 : (yp * 2 + xp + 1) * y2, :] = row

    parts1 = [
        {1: (zc - 1, (-2,)), 0: (0, tuple(range(0, zl, 2))), -1: (0, (zl,))},
        {1: (zc - 1, (-1,)), 0: (0, tuple(range(1, zl, 2)))},
        {1: (zl - LOW0, tuple(range(-LOW0, -2))), -1: (1, tuple(range(zl + 1, WINDOW - LOW0)))},
    ]
    place_of, at = {}, 0
    for part_ in parts1:
        for dz, (_, zs) in part_.items():
            for z in zs:
                place_of[z] = at
                at += 1
    messages = [(k, dz, h) for k, part_ in enumerate(parts1) for dz in part_ for h in range(halves) if dz or h]
    mail = {m: i for i, m in enumerate(messages)}
    moves2 = {-2: (0, zc // 2, 7), -1: (0, zc // 2, 5), 1: (0, zc // 2, 1), 2: (zc // 2 - 1, 1, 0)}
    counts = (EVENS, ODDS)

    def rows(k, dz):
        zs = parts1[k][dz][1]
        return pl.ds(place_of[zs[0]], len(zs))

    def outgoing(k, dz):
        first, zs = parts1[k][dz]
        return (plain if k == 2 else mine.at[k]).at[pl.ds(first, len(zs))]

    for k in (0, 1):
        got[gy, rows(k, 0)] = mine[k]
    for k, part_ in enumerate(parts1):
        for dz, edge in ((1, 0), (-1, gz_n - 1)):
            if dz in part_:

                @pl.when(gz == edge)
                def _(k=k, dz=dz):
                    got[:, rows(k, dz)] = jnp.zeros((gy_n, len(parts1[k][dz][1])) + got.shape[2:], F32)

    def pass_token(round_):
        reach = 2 << round_
        for dz in (-reach, reach):
            when_there(dz, lambda dz=dz: pl.semaphore_signal(
                token.at[round_], inc=1, device_id=(gz + dz, gy), device_id_type=MESH
            ))

    def take_token(round_):
        reach = 2 << round_
        pl.semaphore_wait(token.at[round_], there(-reach).astype(jnp.int32) + there(reach).astype(jnp.int32))

    def each_parity(index, act):
        for parity in (0, 1):
            when(lax.rem(index, 2) == parity, lambda parity=parity: act(parity))

    def edges(act):
        when(gz == 0, lambda: act(0))
        when(gz == gz_n - 1, lambda: act(1))
        when((gz > 0) & (gz < gz_n - 1), lambda: act(None))

    def unpack(k, g):
        for dz in parts1[k]:
            for z in parts1[k][dz][1]:
                for j, (yp, xp) in enumerate(YX):
                    row = got[g, place_of[z], j * y2 : (j + 1) * y2, :]
                    f[z % 2][yp, xp, (z + LOW0) // 2, g * y2 : (g + 1) * y2, :] = row

    def direct(k, dz, h, owner):
        g = lax.rem(gy + 2 * h, gy_n)
        return pltpu.make_async_remote_copy(
            src_ref=outgoing(k, dz),
            dst_ref=got.at[g if owner else gy, rows(k, dz)],
            send_sem=ssem.at[0],
            recv_sem=r1.at[mail[k, dz, (halves - h) % halves if owner else h]],
            device_id=(gz - dz if owner else gz + dz, g),
            device_id_type=MESH,
        )

    def relay(k, dz, h):
        place = got.at[lax.rem(gy + 2 * h, gy_n), rows(k, dz)]
        return pltpu.make_async_remote_copy(
            src_ref=mine.at[k] if dz == 0 and h == 0 else place,
            dst_ref=place,
            send_sem=ssem.at[1],
            recv_sem=rr.at[k],
            device_id=(gz, sibling),
            device_id_type=MESH,
        )

    def wait_rows(sem, n):
        block = got.at[pl.ds(0, halves), pl.ds(0, n)]
        pltpu.make_async_copy(block, block, sem).wait()

    def send(ks):
        def starts(parity):
            far = -1 if parity == 0 else 1
            for k in ks:
                for dz, h in send_order(far, halves):
                    if dz in parts1[k]:
                        when_there(dz, lambda: direct(k, dz, h, False).start())
                if 0 in parts1[k]:
                    relay(k, 0, 0).start()

        each_parity(gz, starts)

    def forward(ks):
        def forwards(parity):
            far = 1 if parity == 0 else -1
            for k in ks:
                for i, (dz, h) in enumerate(receive_order(far, halves)):
                    if k == 0 and ks[0] == 0 and i == 1:
                        send((2,))

                    def go():
                        direct(k, dz, h, True).wait_recv()
                        relay(k, dz, h).start()

                    if dz in parts1[k]:
                        when_there(-dz, go)

        each_parity(gz, forwards)
        each_parity(gy, lambda parity: [unpack(k, g) for k in ks for g in range(parity, gy_n, 2)])

    def height(k, dz):
        return len(parts1[k][dz][1]) if dz in parts1[k] else 0

    def relayed(k):
        total = sum(height(k, dz) for dz in (-1, 0, 1))
        less = (height(k, 1), height(k, -1))
        edges(lambda edge: wait_rows(rr.at[k], total - (0 if edge is None else less[edge])))
        each_parity(gy, lambda parity: [unpack(k, g) for g in range(1 - parity, gy_n, 2)])

    def sent():
        up, down = (sum(height(k, dz) for k in range(3)) for dz in (1, -1))
        own_rows = zl - zl // halves
        edges(lambda edge: wait_rows(ssem.at[0], own_rows + (down if edge != 0 else 0) + (up if edge != 1 else 0)))
        edges(lambda edge: wait_rows(ssem.at[1], zl + (up if edge != 0 else 0) + (down if edge != 1 else 0)))

    rounds = max(gz_n - 2, 1).bit_length() - 1
    pl.semaphore_wait(barrier, count)
    own = LOW0 // 2
    last = own + zc
    send((0, 1))
    forward((0, 1))
    if rounds > 0:
        pass_token(0)
    relayed(0)
    run0(v, f, z0, z_count, 0, own - 1, last + 1, PHASE_A, 0)
    relayed(1)
    run0(v, f, z0, z_count, 1, own - 1, last, PHASE_B, 1)
    run0(v, f, z0, z_count, 0, own, last, PHASE_C, 2)

    here, below, above = pl.ds(own, zc), pl.ds(own - 1, zc), pl.ds(own, zc)
    s = [[ve[yp, xp, here] + vo[yp, xp, below] + vo[yp, xp, above] for xp in (0, 1)] for yp in (0, 1)]
    tall = [s[0][xp] + pair_sum(s[1][xp], 0, 1) for xp in (0, 1)]
    dbuf[...] = fe[0, 0, here] - (27.0 * ve[0, 0, here] - (tall[0] + pair_sum(tall[1], 0, 2)))
    half = gy_n * yc
    for z in range(zc):
        for yp in (0, 1):
            f1[z % 2, 3 + z // 2, yp] = dbuf[z, pl.ds(yp, half, stride=2), :]
    for edge, low, n in ((0, 0, 3), (1, 0, 1), (gz_n - 2, 7, 2), (gz_n - 1, 5, 4)):

        @pl.when(gz == edge)
        def _(low=low, n=n):
            f1[:, low : low + n] = jnp.zeros((2, n) + f1.shape[2:], F32)

    sender = lax.rem(gy, 2) == 1
    def near(zp, dz, target):
        first, n, to = moves2[dz]
        n = min(n, counts[zp] - to)
        return pltpu.make_async_remote_copy(
            src_ref=f1.at[zp, pl.ds(3 + first, n)], dst_ref=f1.at[zp, pl.ds(to, n)],
            send_sem=s2.at[zp], recv_sem=r2.at[zp],
            device_id=(gz + dz, target), device_id_type=MESH,
        )

    def send_near(parity):
        far = -1 if parity == 0 else 1
        for zp in (0, 1):
            for dz in (far, 2 * far, -2 * far, -far):
                when_there(dz, lambda: [near(zp, dz, g).start() for g in (gy, sibling)])

    def wait_near(sem, sign, zps, times):
        def take(missing):
            n = sum(min(moves2[dz][1], counts[zp] - moves2[dz][2]) for zp in zps for dz in moves2 if dz not in missing)
            block = f1.at[pl.ds(0, times), pl.ds(0, n)]
            pltpu.make_async_copy(block, block, sem).wait()

        low_side, high_side = (sign * 2, sign), (-sign * 2, -sign)
        when(gz == 0, lambda: take(low_side))
        when(gz == 1, lambda: take(low_side[:1]))
        when(gz == gz_n - 2, lambda: take(high_side[:1]))
        when(gz == gz_n - 1, lambda: take(high_side))
        when((gz > 1) & (gz < gz_n - 2), lambda: take(()))

    if rounds > 0:
        take_token(0)
    if rounds > 1:
        pass_token(1)
    when(sender, lambda: each_parity(gz, send_near))
    forward((2,))
    relayed(2)
    for phase, odd, ranges in (
        (PHASE_A, 0, ((0, own - 1), (last + 1, EVENS))),
        (PHASE_B, 1, ((0, own - 1), (last, ODDS))),
        (PHASE_C, 0, ((1, own), (last, EVENS - 1))),
    ):
        for low, high in ranges:
            run0(v, f, z0, z_count, odd, low, high, phase, odd if phase is not PHASE_C else 2)
    sent()
    c0, c_count = gz * zc, gz_n * zc
    wait_near(r2.at[0], 1, (0,), 1)
    run1(v1, f1, c0, c_count, 0, 0, EVENS, PHASE_A, 0)
    wait_near(r2.at[1], 1, (1,), 1)
    run1(v1, f1, c0, c_count, 1, 0, ODDS, PHASE_B, 1)
    run1(v1, f1, c0, c_count, 0, 1, EVENS - 1, PHASE_C, 2)

    f2 = []
    for i in range(1, EVENS - 1):
        s = [v1e[yp, pl.ds(i, 1)] + v1o[yp, pl.ds(i - 1, 1)] + v1o[yp, pl.ds(i, 1)] for yp in (0, 1)]
        tall = s[0] + pair_sum(s[1], 0, 1)
        f2.append(f1[0, pl.ds(i, 1), 0] - (27.0 * v1e[0, pl.ds(i, 1)] - (tall + both_sides(tall, 2, 1))))
    q0, q_count = gz * (zc // 2), gz_n * (zc // 2)
    f2e, f2o = f2[0::2], f2[1::2]
    scale2 = [scale_rows(f2[0].shape, q0 - LOW2 + i, q_count) for i in range(7)]
    even2 = [phase2(None, f2e[k], None, scale2[2 * k], PHASE_A) for k in range(4)]
    odd2 = [phase2(None, f2o[k], even2[k] + even2[k + 1], scale2[2 * k + 1], PHASE_B) for k in range(3)]
    for k in (1, 2):
        even2[k] = phase2(even2[k], f2e[k], odd2[k - 1] + odd2[k], scale2[2 * k], PHASE_C)
    v2 = [odd2[0], even2[1], odd2[1], even2[2], odd2[2]]
    in_lane = lax.broadcasted_iota(jnp.int32, v2[0].shape, 2) % 2 == 0
    for k in range(5):
        v1e[0, pl.ds(2 + k, 1)] = v1e[0, pl.ds(2 + k, 1)] + jnp.where(in_lane, v2[k], 0.0)

    run1(v1, f1, c0, c_count, 0, 2, 7, PHASE_A, 2)
    run1(v1, f1, c0, c_count, 1, 2, 6, PHASE_B, 2)
    run1(v1, f1, c0, c_count, 0, 3, 6, PHASE_C, 2)

    for c in range(-1, 6):
        odd = c % 2
        i = (c + LOW1 - odd) // 2
        for yp in (0, 1):
            vc[c + 1, pl.ds(yp, half, stride=2), :] = v1[odd][yp, i]
    ve[0, 0, pl.ds(1, 7)] = ve[0, 0, pl.ds(1, 7)] + vc[...]

    run0(v, f, z0, z_count, 0, 1, 8, PHASE_A, 2)
    run0(v, f, z0, z_count, 1, 1, 7, PHASE_B, 2)
    run0(v, f, z0, z_count, 0, 2, 7, PHASE_C, 2)

    numer = denom = None
    for odd in (0, 1):
        for k in range(zc):
            i = own + k
            here, below, above = pl.ds(i, 1), pl.ds(i - 1 + odd, 1), pl.ds(i + odd, 1)
            p = [[v[odd][yp, xp, here] for xp in (0, 1)] for yp in (0, 1)]
            s = [[p[yp][xp] + v[1 - odd][yp, xp, below] + v[1 - odd][yp, xp, above] for xp in (0, 1)] for yp in (0, 1)]
            b = box0(s)
            for yp, xp in YX:
                image = 27.0 * p[yp][xp] - b[yp][xp]
                numer = add(numer, f[odd][yp, xp, here] * p[yp][xp])
                denom = add(denom, p[yp][xp] * image)
                parity_at = k * 2 + odd
                nat[yp, xp, pl.ds(parity_at, 1)] = image
    rows = numer.shape[1]
    for j, total in enumerate((numer, denom)):
        acc = None
        for r in range(0, rows, 8):
            acc = add(acc, total[0, r : r + 8, :])
        part[pl.ds(j, 1), :] = jnp.sum(acc, axis=0, keepdims=True)

    for r in range(1, rounds):
        take_token(r)
        if r + 1 < rounds:
            pass_token(r + 1)

    def spread(to, target):
        return pltpu.make_async_remote_copy(
            src_ref=part, dst_ref=parts.at[gz], send_sem=rs, recv_sem=r3,
            device_id=(to, target), device_id_type=MESH,
        )

    @pl.when(sender)
    def _():
        for to in range(gz_n):

            def go():
                for g in (sibling, gy):
                    spread(to, g).start()

            when(gz != to, go)

    parts[gz] = part[...]

    back = permutation(nx, True)
    for which, out in ((0, sol_ref), (1, res_ref)):
        for z in range(zl):
            for yp, xp in YX:
                if which == 0:
                    row = v[z % 2][yp, xp, own + z // 2, pl.ds(gy * y2, y2), :]
                else:
                    row = nat[yp, xp, z, pl.ds(gy * y2, y2), :]
                flat[xp, pl.ds(z * yl + yp, y2, stride=2), :] = row
        out[...] = jnp.dot(
            jnp.concatenate([flat[0], flat[1]], axis=1), back, precision=lax.Precision.HIGHEST, preferred_element_type=F32
        ).reshape(zl, yl, nx)

    others = parts.at[pl.ds(0, gz_n - 1)]
    pltpu.make_async_copy(others, others, r3).wait()
    when(sender, lambda: [wait_near(s2.at[zp], -1, (zp,), 2) for zp in (0, 1)])
    when(sender, lambda: [pltpu.make_async_copy(others, others, rs).wait() for _ in range(2)])
    sums = parts[0]
    for d in range(1, gz_n):
        sums = sums + parts[d]
    alpha = jnp.sum(sums[0:1], axis=1, keepdims=True) / jnp.sum(sums[1:2], axis=1, keepdims=True)
    alpha_ref[...] = jnp.broadcast_to(alpha.reshape(1, 1), alpha_ref.shape)


def solution(mesh):
    gz_n, gy_n = mesh.shape["gz"], mesh.shape["gy"]

    def body(rhs):
        zl, yl, nx = rhs.shape
        y2, x2 = yl // 2, nx // 2
        y_half = gy_n * y2
        zc, yc = zl // 2, y2 // 2
        vmem = lambda *shape: pltpu.VMEM(shape, F32)
        dma = lambda *shape: pltpu.SemaphoreType.DMA(shape)
        p, image, alpha = pl.pallas_call(
            functools.partial(kernel, gz_n, gy_n),
            out_shape=[vmem(*rhs.shape)] * 2 + [vmem(yl, nx)],
            in_specs=[pl.BlockSpec(memory_space=pl.ANY)],
            out_specs=[pl.BlockSpec(memory_space=pltpu.VMEM)] * 3,
            scratch_shapes=[
                vmem(2, zl * yl, x2),
                vmem(2, zc, 4 * y2, x2),
                vmem(zl, 4 * y2, x2),
                vmem(gy_n, WINDOW, 4 * y2, x2),
                vmem(2, 2, EVENS, y_half, x2),
                vmem(2, 2, ODDS, y_half, x2),
                vmem(2, 2, EVENS, y_half, x2),
                vmem(2, 2, ODDS, y_half, x2),
                vmem(zc, y_half, x2),
                vmem(2, EVENS, 2, gy_n * yc, x2),
                vmem(2, EVENS, gy_n * yc, x2),
                vmem(2, ODDS, gy_n * yc, x2),
                vmem(7, y_half, x2),
                vmem(2, x2),
                vmem(gz_n, 2, x2),
                vmem(2, 2, zl, y_half, x2),
                dma(2), dma(7 * (gy_n // 2) - 2), dma(3), dma(2), dma(2),
                pltpu.SemaphoreType.DMA, pltpu.SemaphoreType.DMA,
                vmem(zl, yl, nx), pltpu.SemaphoreType.DMA,
                pltpu.SemaphoreType.REGULAR((max(1, max(gz_n - 2, 1).bit_length() - 1),)),
            ],
            compiler_params=pltpu.CompilerParams(has_side_effects=True, collective_id=0),
        )(rhs)
        return p * alpha, rhs - image * alpha

    return jax.shard_map(
        lambda rhs: tuple(body(rhs)),
        mesh=mesh,
        in_specs=(P("gz", "gy", None),),
        out_specs=(P("gz", "gy", None), P("gz", "gy", None)),
        check_vma=False,
    )
```

```python
import functools

import jax
import jax.numpy as jnp
from jax import lax
from jax.experimental import pallas as pl
from jax.experimental.pallas import tpu as pltpu
from jax.sharding import PartitionSpec as P

MESH = pl.DeviceIdType.MESH
F32 = jnp.float32

LOW0, LOW1, LOW2 = 4, 6, 2
EVENS, ODDS = 9, 8
WINDOW = EVENS + ODDS

PHASE_A = ((0, (0, 1)), (1, (0, 1)))
PHASE_B = ((0, (0, 1)), (1, (0, 1, 0)), (0, (1, 0)))
PHASE_C = ((1, (1, 0)), (0, (1, 0)))

CHUNK0 = 3
CHUNK1 = 9


def add(*terms):
    total = None
    for term in terms:
        if term is not None:
            total = term if total is None else total + term
    return total


def shift(x, axis, step):
    if x is None:
        return None
    size = x.shape[axis]
    moved = pltpu.roll(x, step % size, axis)
    index = lax.broadcasted_iota(jnp.int32, x.shape, axis)
    keep = index >= step if step > 0 else index < size + step
    return jnp.where(keep, moved, 0.0)


def pair_sum(other, parity, axis):
    return add(other, shift(other, axis, 1 if parity == 0 else -1))


def both_sides(x, axis, step):
    return add(shift(x, axis, step), shift(x, axis, -step))


def scale_rows(shape, first, count):
    row = first + 2 * lax.broadcasted_iota(jnp.int32, shape, 0)
    return jnp.where((row >= 0) & (row < count), F32(1.0 / 26.0), F32(0.0))


def box0(s):
    tall = [[add(s[yp][xp], pair_sum(s[1 - yp][xp], yp, 1)) for xp in (0, 1)] for yp in (0, 1)]
    return [[add(tall[yp][xp], pair_sum(tall[yp][1 - xp], xp, 2)) for xp in (0, 1)] for yp in (0, 1)]


def edge_some(x, axis, width, inner, outer, at_start, at_end):
    size = x.shape[axis]
    index = lax.broadcasted_iota(jnp.int32, x.shape, axis)
    edge = (index < width) if at_start else None
    if at_end:
        last = index >= size - width
        edge = last if edge is None else edge | last
    return x * jnp.where(edge, F32(outer), F32(inner))


def phase0(v, f, zs, scale, steps):
    v = [list(v[0]), list(v[1])]
    for yp, order in steps:
        w = [add(zs[yp][xp], pair_sum(add(zs[1 - yp][xp], v[1 - yp][xp]), yp, 1)) for xp in (0, 1)]
        a, b = order[0], order[1]
        near, far = (1, -1) if a == 0 else (-1, 1)
        u = add(w[b], v[yp][b])
        h = add(f[yp][a], w[a])
        q = add(w[a], h * scale)
        y_far = shift(q if u is None else q + u * scale, 2, far)
        if u is None:
            v[yp][a] = h * scale
            v[yp][b] = add(f[yp][b], w[b], q, y_far) * scale
            continue
        u_near = shift(u, 2, near)
        if len(order) == 3:
            p = add(w[b], add(f[yp][b], w[b]) * scale)
            x_near = shift(p + scale * (q + F32(3.0) * (scale * u)), 2, near)
            thrice = edge_some(u, 2, 1, 3.0, 2.0, True, True) + shift(u, 2, 2 * near)
            inner = edge_some(q, 2, 1, 2.0, 1.0, a == 0, a == 1) + y_far + scale * thrice
            v[yp][a] = add(h, p, x_near, scale * inner) * scale
        else:
            v[yp][a] = add(h, u, u_near) * scale
        twice = edge_some(u, 2, 1, 2.0, 1.0, a == 1, a == 0) + u_near
        v[yp][b] = add(f[yp][b], w[b], q, y_far, twice * scale) * scale
    return v


def box1(s):
    tall = [add(s[yp], pair_sum(s[1 - yp], yp, 1)) for yp in (0, 1)]
    return [add(t, both_sides(t, 2, 1)) for t in tall]


def line_pair(v, g, w, scale, parity, order, step):
    a, b = order[0], order[1]
    first = parity == a
    h = add(g, w)
    u = add(w, v)
    q = add(w, h * scale)
    if u is None:
        return add(h, both_sides(jnp.where(first, q, 0.0), 2, step)) * scale
    m = jnp.where(first, q, u)
    second = add(edge_some(m, 2, step, 2.0, 1.0, True, True), both_sides(m, 2, 2 * step)) * scale
    if len(order) == 2:
        return add(h, both_sides(m, 2, step), jnp.where(first, 0.0, second)) * scale
    here, there = (-step, step) if a == 0 else (step, -step)
    index = lax.broadcasted_iota(jnp.int32, scale.shape, 2)
    ends = (index < 2 * step) | (index >= scale.shape[2] - 2 * step)
    square = scale * scale
    some = square * u
    m_here = jnp.where(first, q, q + some * jnp.where(ends, F32(2.0), F32(3.0)))
    m_there = jnp.where(first, q, q + some * F32(3.0))
    third = jnp.where(first, square * both_sides(u, 2, 3 * step), 0.0)
    return add(h, shift(m_here, 2, here), shift(m_there, 2, there), second, third) * scale


def phase1(v, g, zs, scale, steps):
    v = list(v)
    parity = lax.broadcasted_iota(jnp.int32, scale.shape, 2) % 2
    for yp, order in steps:
        w = add(zs[yp], pair_sum(add(zs[1 - yp], v[1 - yp]), yp, 1))
        v[yp] = line_pair(v[yp], g[yp], w, scale, parity, order, 1)
    return v


def phase2(v, g, zs, scale, steps):
    shape = scale.shape
    y_par = lax.broadcasted_iota(jnp.int32, shape, 1) % 2
    x_par = (lax.broadcasted_iota(jnp.int32, shape, 2) // 2) % 2
    for yp, order in steps:
        w = add(zs, both_sides(add(zs, v), 1, 1))
        new = line_pair(v, g, w, scale, x_par, order, 2)
        v = jnp.where(y_par == yp, new, 0.0 if v is None else v)
    return v


def chunks(low, high, size):
    for start in range(low, high, size):
        yield start, min(size, high - start)


YX = [(0, 0), (0, 1), (1, 0), (1, 1)]


NONE = [[None, None], [None, None]]


def run0(v, f, z0, z_count, odd, low, high, steps, fresh):
    for at, n in chunks(low, high, CHUNK0):
        here = pl.ds(at, n)
        below, above = (pl.ds(at, n), pl.ds(at + 1, n)) if odd else (pl.ds(at - 1, n), pl.ds(at, n))
        rhs = [[f[odd][yp, xp, here] for xp in (0, 1)] for yp in (0, 1)]
        scale = scale_rows(rhs[0][0].shape, z0 + 2 * at - LOW0 + odd, z_count)
        zs, old = NONE, NONE
        if fresh > 0:
            zs = [[v[1 - odd][yp, xp, below] + v[1 - odd][yp, xp, above] for xp in (0, 1)] for yp in (0, 1)]
        if fresh > 1:
            old = [[v[odd][yp, xp, here] for xp in (0, 1)] for yp in (0, 1)]
        new = phase0(old, rhs, zs, scale, steps)
        for yp, xp in YX:
            v[odd][yp, xp, here] = new[yp][xp]


def run1(v, f, z0, z_count, odd, low, high, steps, fresh):
    for at, n in chunks(low, high, CHUNK1):
        here = pl.ds(at, n)
        below, above = (pl.ds(at, n), pl.ds(at + 1, n)) if odd else (pl.ds(at - 1, n), pl.ds(at, n))
        g = [f[odd, here, yp] for yp in (0, 1)]
        scale = scale_rows(g[0].shape, z0 + 2 * at - LOW1 + odd, z_count)
        zs, old = NONE[0], NONE[0]
        if fresh > 0:
            zs = [v[1 - odd][yp, below] + v[1 - odd][yp, above] for yp in (0, 1)]
        if fresh > 1:
            old = [v[odd][yp, here] for yp in (0, 1)]
        new = phase1(old, g, zs, scale, steps)
        for yp in (0, 1):
            v[odd][yp, here] = new[yp]


def permutation(size, inverse):
    half = size // 2
    wide = lax.broadcasted_iota(jnp.int32, (size, size), 0 if inverse else 1)
    tall = lax.broadcasted_iota(jnp.int32, (size, size), 1 if inverse else 0)
    source = jnp.where(wide < half, 2 * wide, 2 * (wide - half) + 1)
    return jnp.where(tall == source, F32(1.0), F32(0.0))


def when(condition, act):
    @pl.when(condition)
    def _():
        act()


def send_order(far, halves):
    order = [(dz, h) for dz in (0, far, -far) for h in reversed(range(halves))]
    return [(dz, h) for dz, h in order if dz != 0 or h != 0]


def receive_order(far, halves):
    order = [(dz, h) for h in range(halves) for dz in (0, -far, far)]
    return [(dz, h) for dz, h in order if dz != 0 or h != 0]


def kernel(
    gz_n, gy_n, rhs_hbm, sol_ref, res_ref, alpha_ref,
    flat, mine, plain, got, fe, fo, ve, vo, dbuf, f1, v1e, v1o, vc, part, parts, nat,
    ssem, r1, rr, s2, r2, r3, rs, rhs_ref, s5, token,
):
    gz, gy = lax.axis_index("gz"), lax.axis_index("gy")
    zl, yl, nx = rhs_ref.shape
    fetch = pltpu.make_async_copy(rhs_hbm, rhs_ref, s5)
    fetch.start()
    y2, x2 = yl // 2, nx // 2
    yc = y2 // 2
    zc = zl // 2
    z_count = gz_n * zl
    z0 = gz * zl
    f, v = (fe, fo), (ve, vo)
    v1 = (v1e, v1o)
    halves = gy_n // 2
    sibling = gy + 1 - 2 * lax.rem(gy, 2)

    def there(dz):
        return (gz + dz >= 0) & (gz + dz < gz_n)

    def when_there(dz, go):
        if dz == 0:
            go()
        else:
            when(there(dz), go)

    barrier = pltpu.get_barrier_semaphore()
    count = jnp.int32(0)
    greet = [(dz, 2 * h) for h in reversed(range(halves)) for dz in (-1, 1)] + [(-2, 0), (2, 0)] + [(0, dg) for dg in range(1, gy_n)]
    greet = [(dz, dg, gy) for dz, dg in greet] + [(dz, 2 * h, sibling) for h in range(1, halves) for dz in (-1, 1)]
    for dz, dg, base in greet:

        def go(dz=dz, dg=dg, base=base):
            pl.semaphore_signal(
                barrier, inc=1, device_id=(gz + dz, lax.rem(base + dg, gy_n)), device_id_type=MESH
            )

        when_there(dz, go)
        count = count + (1 if dz == 0 else there(dz).astype(jnp.int32))

    fetch.wait()
    lane = lax.broadcasted_iota(jnp.int32, (zl * yl, x2), 1)
    source = 2 * lax.rem(lane, x2 // 2)
    rows = rhs_ref[...].reshape(zl * yl, nx)
    for xp in (0, 1):
        left, right = (
            jnp.take_along_axis(rows[:, i : i + x2], source + xp, axis=1, mode="promise_in_bounds") for i in (0, x2)
        )
        flat[xp] = jnp.where(lane < x2 // 2, left, right)
    for z in range(zl):
        for yp, xp in YX:
            row = flat[xp, pl.ds(z * yl + yp, y2, stride=2), :]
            mine[z % 2, z // 2, (yp * 2 + xp) * y2 : (yp * 2 + xp + 1) * y2, :] = row
            plain[z, (yp * 2 + xp) * y2 : (yp * 2 + xp + 1) * y2, :] = row

    parts1 = [
        {1: (zc - 1, (-2,)), 0: (0, tuple(range(0, zl, 2))), -1: (0, (zl,))},
        {1: (zc - 1, (-1,)), 0: (0, tuple(range(1, zl, 2)))},
        {1: (zl - LOW0, tuple(range(-LOW0, -2))), -1: (1, tuple(range(zl + 1, WINDOW - LOW0)))},
    ]
    place_of, at = {}, 0
    for part_ in parts1:
        for dz, (_, zs) in part_.items():
            for z in zs:
                place_of[z] = at
                at += 1
    messages = [(k, dz, h) for k, part_ in enumerate(parts1) for dz in part_ for h in range(halves) if dz or h]
    mail = {m: i for i, m in enumerate(messages)}
    moves2 = {-2: (0, zc // 2, 7), -1: (0, zc // 2, 5), 1: (0, zc // 2, 1), 2: (zc // 2 - 1, 1, 0)}
    counts = (EVENS, ODDS)

    def rows(k, dz):
        zs = parts1[k][dz][1]
        return pl.ds(place_of[zs[0]], len(zs))

    def outgoing(k, dz):
        first, zs = parts1[k][dz]
        return (plain if k == 2 else mine.at[k]).at[pl.ds(first, len(zs))]

    for k in (0, 1):
        got[gy, rows(k, 0)] = mine[k]
    for k, part_ in enumerate(parts1):
        for dz, edge in ((1, 0), (-1, gz_n - 1)):
            if dz in part_:

                @pl.when(gz == edge)
                def _(k=k, dz=dz):
                    got[:, rows(k, dz)] = jnp.zeros((gy_n, len(parts1[k][dz][1])) + got.shape[2:], F32)

    def pass_token(round_):
        reach = 2 << round_
        for dz in (-reach, reach):
            when_there(dz, lambda dz=dz: pl.semaphore_signal(
                token.at[round_], inc=1, device_id=(gz + dz, gy), device_id_type=MESH
            ))

    def take_token(round_):
        reach = 2 << round_
        pl.semaphore_wait(token.at[round_], there(-reach).astype(jnp.int32) + there(reach).astype(jnp.int32))

    def each_parity(index, act):
        for parity in (0, 1):
            when(lax.rem(index, 2) == parity, lambda parity=parity: act(parity))

    def edges(act):
        when(gz == 0, lambda: act(0))
        when(gz == gz_n - 1, lambda: act(1))
        when((gz > 0) & (gz < gz_n - 1), lambda: act(None))

    def unpack(k, g):
        for dz in parts1[k]:
            for z in parts1[k][dz][1]:
                for j, (yp, xp) in enumerate(YX):
                    row = got[g, place_of[z], j * y2 : (j + 1) * y2, :]
                    f[z % 2][yp, xp, (z + LOW0) // 2, g * y2 : (g + 1) * y2, :] = row

    def direct(k, dz, h, owner):
        g = lax.rem(gy + 2 * h, gy_n)
        return pltpu.make_async_remote_copy(
            src_ref=outgoing(k, dz),
            dst_ref=got.at[g if owner else gy, rows(k, dz)],
            send_sem=ssem.at[0],
            recv_sem=r1.at[mail[k, dz, (halves - h) % halves if owner else h]],
            device_id=(gz - dz if owner else gz + dz, g),
            device_id_type=MESH,
        )

    def relay(k, dz, h):
        place = got.at[lax.rem(gy + 2 * h, gy_n), rows(k, dz)]
        return pltpu.make_async_remote_copy(
            src_ref=mine.at[k] if dz == 0 and h == 0 else place,
            dst_ref=place,
            send_sem=ssem.at[1],
            recv_sem=rr.at[k],
            device_id=(gz, sibling),
            device_id_type=MESH,
        )

    def wait_rows(sem, n):
        block = got.at[pl.ds(0, halves), pl.ds(0, n)]
        pltpu.make_async_copy(block, block, sem).wait()

    def send(ks):
        def starts(parity):
            far = -1 if parity == 0 else 1
            for k in ks:
                for dz, h in send_order(far, halves):
                    if dz in parts1[k]:
                        when_there(dz, lambda: direct(k, dz, h, False).start())
                if 0 in parts1[k]:
                    relay(k, 0, 0).start()

        each_parity(gz, starts)

    def forward(ks):
        def forwards(parity):
            far = 1 if parity == 0 else -1
            for k in ks:
                for i, (dz, h) in enumerate(receive_order(far, halves)):
                    if k == 0 and ks[0] == 0 and i == 1:
                        send((2,))

                    def go():
                        direct(k, dz, h, True).wait_recv()
                        relay(k, dz, h).start()

                    if dz in parts1[k]:
                        when_there(-dz, go)

        each_parity(gz, forwards)
        each_parity(gy, lambda parity: [unpack(k, g) for k in ks for g in range(parity, gy_n, 2)])

    def height(k, dz):
        return len(parts1[k][dz][1]) if dz in parts1[k] else 0

    def relayed(k):
        total = sum(height(k, dz) for dz in (-1, 0, 1))
        less = (height(k, 1), height(k, -1))
        edges(lambda edge: wait_rows(rr.at[k], total - (0 if edge is None else less[edge])))
        each_parity(gy, lambda parity: [unpack(k, g) for g in range(1 - parity, gy_n, 2)])

    def sent():
        up, down = (sum(height(k, dz) for k in range(3)) for dz in (1, -1))
        own_rows = zl - zl // halves
        edges(lambda edge: wait_rows(ssem.at[0], own_rows + (down if edge != 0 else 0) + (up if edge != 1 else 0)))
        edges(lambda edge: wait_rows(ssem.at[1], zl + (up if edge != 0 else 0) + (down if edge != 1 else 0)))

    rounds = max(gz_n - 2, 1).bit_length() - 1
    pl.semaphore_wait(barrier, count)
    own = LOW0 // 2
    last = own + zc
    send((0, 1))
    forward((0, 1))
    if rounds > 0:
        pass_token(0)
    relayed(0)
    run0(v, f, z0, z_count, 0, own - 1, last + 1, PHASE_A, 0)
    relayed(1)
    run0(v, f, z0, z_count, 1, own - 1, last, PHASE_B, 1)
    run0(v, f, z0, z_count, 0, own, last, PHASE_C, 2)

    here, below, above = pl.ds(own, zc), pl.ds(own - 1, zc), pl.ds(own, zc)
    s = [[ve[yp, xp, here] + vo[yp, xp, below] + vo[yp, xp, above] for xp in (0, 1)] for yp in (0, 1)]
    tall = [s[0][xp] + pair_sum(s[1][xp], 0, 1) for xp in (0, 1)]
    dbuf[...] = fe[0, 0, here] - (27.0 * ve[0, 0, here] - (tall[0] + pair_sum(tall[1], 0, 2)))
    half = gy_n * yc
    for z in range(zc):
        for yp in (0, 1):
            f1[z % 2, 3 + z // 2, yp] = dbuf[z, pl.ds(yp, half, stride=2), :]
    for edge, low, n in ((0, 0, 3), (1, 0, 1), (gz_n - 2, 7, 2), (gz_n - 1, 5, 4)):

        @pl.when(gz == edge)
        def _(low=low, n=n):
            f1[:, low : low + n] = jnp.zeros((2, n) + f1.shape[2:], F32)

    sender = lax.rem(gy, 2) == 1
    def near(zp, dz, target):
        first, n, to = moves2[dz]
        n = min(n, counts[zp] - to)
        return pltpu.make_async_remote_copy(
            src_ref=f1.at[zp, pl.ds(3 + first, n)], dst_ref=f1.at[zp, pl.ds(to, n)],
            send_sem=s2.at[zp], recv_sem=r2.at[zp],
            device_id=(gz + dz, target), device_id_type=MESH,
        )

    def send_near(parity):
        far = -1 if parity == 0 else 1
        for zp in (0, 1):
            for dz in (far, 2 * far, -2 * far, -far):
                when_there(dz, lambda: [near(zp, dz, g).start() for g in (gy, sibling)])

    def wait_near(sem, sign, zps, times):
        def take(missing):
            n = sum(min(moves2[dz][1], counts[zp] - moves2[dz][2]) for zp in zps for dz in moves2 if dz not in missing)
            block = f1.at[pl.ds(0, times), pl.ds(0, n)]
            pltpu.make_async_copy(block, block, sem).wait()

        low_side, high_side = (sign * 2, sign), (-sign * 2, -sign)
        when(gz == 0, lambda: take(low_side))
        when(gz == 1, lambda: take(low_side[:1]))
        when(gz == gz_n - 2, lambda: take(high_side[:1]))
        when(gz == gz_n - 1, lambda: take(high_side))
        when((gz > 1) & (gz < gz_n - 2), lambda: take(()))

    if rounds > 0:
        take_token(0)
    if rounds > 1:
        pass_token(1)
    when(sender, lambda: each_parity(gz, send_near))
    forward((2,))
    relayed(2)
    for phase, odd, ranges in (
        (PHASE_A, 0, ((0, own - 1), (last + 1, EVENS))),
        (PHASE_B, 1, ((0, own - 1), (last, ODDS))),
        (PHASE_C, 0, ((1, own), (last, EVENS - 1))),
    ):
        for low, high in ranges:
            run0(v, f, z0, z_count, odd, low, high, phase, odd if phase is not PHASE_C else 2)
    sent()
    c0, c_count = gz * zc, gz_n * zc
    wait_near(r2.at[0], 1, (0,), 1)
    run1(v1, f1, c0, c_count, 0, 0, EVENS, PHASE_A, 0)
    wait_near(r2.at[1], 1, (1,), 1)
    run1(v1, f1, c0, c_count, 1, 0, ODDS, PHASE_B, 1)
    run1(v1, f1, c0, c_count, 0, 1, EVENS - 1, PHASE_C, 2)

    f2 = []
    for i in range(1, EVENS - 1):
        s = [v1e[yp, pl.ds(i, 1)] + v1o[yp, pl.ds(i - 1, 1)] + v1o[yp, pl.ds(i, 1)] for yp in (0, 1)]
        tall = s[0] + pair_sum(s[1], 0, 1)
        f2.append(f1[0, pl.ds(i, 1), 0] - (27.0 * v1e[0, pl.ds(i, 1)] - (tall + both_sides(tall, 2, 1))))
    q0, q_count = gz * (zc // 2), gz_n * (zc // 2)
    f2e, f2o = f2[0::2], f2[1::2]
    scale2 = [scale_rows(f2[0].shape, q0 - LOW2 + i, q_count) for i in range(7)]
    even2 = [phase2(None, f2e[k], None, scale2[2 * k], PHASE_A) for k in range(4)]
    odd2 = [phase2(None, f2o[k], even2[k] + even2[k + 1], scale2[2 * k + 1], PHASE_B) for k in range(3)]
    for k in (1, 2):
        even2[k] = phase2(even2[k], f2e[k], odd2[k - 1] + odd2[k], scale2[2 * k], PHASE_C)
    v2 = [odd2[0], even2[1], odd2[1], even2[2], odd2[2]]
    in_lane = lax.broadcasted_iota(jnp.int32, v2[0].shape, 2) % 2 == 0
    for k in range(5):
        v1e[0, pl.ds(2 + k, 1)] = v1e[0, pl.ds(2 + k, 1)] + jnp.where(in_lane, v2[k], 0.0)

    run1(v1, f1, c0, c_count, 0, 2, 7, PHASE_A, 2)
    run1(v1, f1, c0, c_count, 1, 2, 6, PHASE_B, 2)
    run1(v1, f1, c0, c_count, 0, 3, 6, PHASE_C, 2)

    for c in range(-1, 6):
        odd = c % 2
        i = (c + LOW1 - odd) // 2
        for yp in (0, 1):
            vc[c + 1, pl.ds(yp, half, stride=2), :] = v1[odd][yp, i]
    ve[0, 0, pl.ds(1, 7)] = ve[0, 0, pl.ds(1, 7)] + vc[...]

    run0(v, f, z0, z_count, 0, 1, 8, PHASE_A, 2)
    run0(v, f, z0, z_count, 1, 1, 7, PHASE_B, 2)
    run0(v, f, z0, z_count, 0, 2, 7, PHASE_C, 2)

    numer = denom = None
    for odd in (0, 1):
        for k in range(zc):
            i = own + k
            here, below, above = pl.ds(i, 1), pl.ds(i - 1 + odd, 1), pl.ds(i + odd, 1)
            p = [[v[odd][yp, xp, here] for xp in (0, 1)] for yp in (0, 1)]
            s = [[p[yp][xp] + v[1 - odd][yp, xp, below] + v[1 - odd][yp, xp, above] for xp in (0, 1)] for yp in (0, 1)]
            b = box0(s)
            for yp, xp in YX:
                image = 27.0 * p[yp][xp] - b[yp][xp]
                numer = add(numer, f[odd][yp, xp, here] * p[yp][xp])
                denom = add(denom, p[yp][xp] * image)
                parity_at = k * 2 + odd
                nat[yp, xp, pl.ds(parity_at, 1)] = image
    rows = numer.shape[1]
    for j, total in enumerate((numer, denom)):
        acc = None
        for r in range(0, rows, 8):
            acc = add(acc, total[0, r : r + 8, :])
        part[pl.ds(j, 1), :] = jnp.sum(acc, axis=0, keepdims=True)

    for r in range(1, rounds):
        take_token(r)
        if r + 1 < rounds:
            pass_token(r + 1)

    def spread(to, target):
        return pltpu.make_async_remote_copy(
            src_ref=part, dst_ref=parts.at[gz], send_sem=rs, recv_sem=r3,
            device_id=(to, target), device_id_type=MESH,
        )

    @pl.when(sender)
    def _():
        for to in range(gz_n):

            def go():
                for g in (sibling, gy):
                    spread(to, g).start()

            when(gz != to, go)

    parts[gz] = part[...]

    back = permutation(nx, True)
    for which, out in ((0, sol_ref), (1, res_ref)):
        for z in range(zl):
            for yp, xp in YX:
                if which == 0:
                    row = v[z % 2][yp, xp, own + z // 2, pl.ds(gy * y2, y2), :]
                else:
                    row = nat[yp, xp, z, pl.ds(gy * y2, y2), :]
                flat[xp, pl.ds(z * yl + yp, y2, stride=2), :] = row
        out[...] = jnp.dot(
            jnp.concatenate([flat[0], flat[1]], axis=1), back, precision=lax.Precision.HIGHEST, preferred_element_type=F32
        ).reshape(zl, yl, nx)

    others = parts.at[pl.ds(0, gz_n - 1)]
    pltpu.make_async_copy(others, others, r3).wait()
    when(sender, lambda: [wait_near(s2.at[zp], -1, (zp,), 2) for zp in (0, 1)])
    when(sender, lambda: [pltpu.make_async_copy(others, others, rs).wait() for _ in range(2)])
    sums = parts[0]
    for d in range(1, gz_n):
        sums = sums + parts[d]
    alpha = jnp.sum(sums[0:1], axis=1, keepdims=True) / jnp.sum(sums[1:2], axis=1, keepdims=True)
    alpha_ref[...] = jnp.broadcast_to(alpha.reshape(1, 1), alpha_ref.shape)


def solution(mesh):
    gz_n, gy_n = mesh.shape["gz"], mesh.shape["gy"]

    def body(rhs):
        zl, yl, nx = rhs.shape
        y2, x2 = yl // 2, nx // 2
        y_half = gy_n * y2
        zc, yc = zl // 2, y2 // 2
        vmem = lambda *shape: pltpu.VMEM(shape, F32)
        dma = lambda *shape: pltpu.SemaphoreType.DMA(shape)
        p, image, alpha = pl.pallas_call(
            functools.partial(kernel, gz_n, gy_n),
            out_shape=[vmem(*rhs.shape)] * 2 + [vmem(yl, nx)],
            in_specs=[pl.BlockSpec(memory_space=pl.ANY)],
            out_specs=[pl.BlockSpec(memory_space=pltpu.VMEM)] * 3,
            scratch_shapes=[
                vmem(2, zl * yl, x2),
                vmem(2, zc, 4 * y2, x2),
                vmem(zl, 4 * y2, x2),
                vmem(gy_n, WINDOW, 4 * y2, x2),
                vmem(2, 2, EVENS, y_half, x2),
                vmem(2, 2, ODDS, y_half, x2),
                vmem(2, 2, EVENS, y_half, x2),
                vmem(2, 2, ODDS, y_half, x2),
                vmem(zc, y_half, x2),
                vmem(2, EVENS, 2, gy_n * yc, x2),
                vmem(2, EVENS, gy_n * yc, x2),
                vmem(2, ODDS, gy_n * yc, x2),
                vmem(7, y_half, x2),
                vmem(2, x2),
                vmem(gz_n, 2, x2),
                vmem(2, 2, zl, y_half, x2),
                dma(2), dma(7 * (gy_n // 2) - 2), dma(3), dma(2), dma(2),
                pltpu.SemaphoreType.DMA, pltpu.SemaphoreType.DMA,
                vmem(zl, yl, nx), pltpu.SemaphoreType.DMA,
                pltpu.SemaphoreType.REGULAR((max(1, max(gz_n - 2, 1).bit_length() - 1),)),
            ],
            compiler_params=pltpu.CompilerParams(has_side_effects=True, collective_id=0),
        )(rhs)
        return p * alpha, rhs - image * alpha

    return jax.shard_map(
        lambda rhs: tuple(body(rhs)),
        mesh=mesh,
        in_specs=(P("gz", "gy", None),),
        out_specs=(P("gz", "gy", None), P("gz", "gy", None)),
        check_vma=False,
    )
```

```python
import functools

import jax
import jax.numpy as jnp
from jax import lax
from jax.experimental import pallas as pl
from jax.experimental.pallas import tpu as pltpu
from jax.sharding import PartitionSpec as P

MESH = pl.DeviceIdType.MESH
F32 = jnp.float32

LOW0, LOW1, LOW2 = 4, 6, 2
EVENS, ODDS = 9, 8
WINDOW = EVENS + ODDS

PHASE_A = ((0, (0, 1)), (1, (0, 1)))
PHASE_B = ((0, (0, 1)), (1, (0, 1, 0)), (0, (1, 0)))
PHASE_C = ((1, (1, 0)), (0, (1, 0)))

CHUNK0 = 3
CHUNK1 = 9


def add(*terms):
    total = None
    for term in terms:
        if term is not None:
            total = term if total is None else total + term
    return total


def shift(x, axis, step):
    if x is None:
        return None
    size = x.shape[axis]
    moved = pltpu.roll(x, step % size, axis)
    index = lax.broadcasted_iota(jnp.int32, x.shape, axis)
    keep = index >= step if step > 0 else index < size + step
    return jnp.where(keep, moved, 0.0)


def pair_sum(other, parity, axis):
    return add(other, shift(other, axis, 1 if parity == 0 else -1))


def both_sides(x, axis, step):
    return add(shift(x, axis, step), shift(x, axis, -step))


def scale_rows(shape, first, count):
    row = first + 2 * lax.broadcasted_iota(jnp.int32, shape, 0)
    return jnp.where((row >= 0) & (row < count), F32(1.0 / 26.0), F32(0.0))


def box0(s):
    tall = [[add(s[yp][xp], pair_sum(s[1 - yp][xp], yp, 1)) for xp in (0, 1)] for yp in (0, 1)]
    return [[add(tall[yp][xp], pair_sum(tall[yp][1 - xp], xp, 2)) for xp in (0, 1)] for yp in (0, 1)]


def edge_some(x, axis, width, inner, outer, at_start, at_end):
    size = x.shape[axis]
    index = lax.broadcasted_iota(jnp.int32, x.shape, axis)
    edge = (index < width) if at_start else None
    if at_end:
        last = index >= size - width
        edge = last if edge is None else edge | last
    return x * jnp.where(edge, F32(outer), F32(inner))


def phase0(v, f, zs, scale, steps):
    v = [list(v[0]), list(v[1])]
    for yp, order in steps:
        w = [add(zs[yp][xp], pair_sum(add(zs[1 - yp][xp], v[1 - yp][xp]), yp, 1)) for xp in (0, 1)]
        a, b = order[0], order[1]
        near, far = (1, -1) if a == 0 else (-1, 1)
        u = add(w[b], v[yp][b])
        h = add(f[yp][a], w[a])
        q = add(w[a], h * scale)
        y_far = shift(q if u is None else q + u * scale, 2, far)
        if u is None:
            v[yp][a] = h * scale
            v[yp][b] = add(f[yp][b], w[b], q, y_far) * scale
            continue
        u_near = shift(u, 2, near)
        if len(order) == 3:
            p = add(w[b], add(f[yp][b], w[b]) * scale)
            x_near = shift(p + scale * (q + F32(3.0) * (scale * u)), 2, near)
            thrice = edge_some(u, 2, 1, 3.0, 2.0, True, True) + shift(u, 2, 2 * near)
            inner = edge_some(q, 2, 1, 2.0, 1.0, a == 0, a == 1) + y_far + scale * thrice
            v[yp][a] = add(h, p, x_near, scale * inner) * scale
        else:
            v[yp][a] = add(h, u, u_near) * scale
        twice = edge_some(u, 2, 1, 2.0, 1.0, a == 1, a == 0) + u_near
        v[yp][b] = add(f[yp][b], w[b], q, y_far, twice * scale) * scale
    return v


def box1(s):
    tall = [add(s[yp], pair_sum(s[1 - yp], yp, 1)) for yp in (0, 1)]
    return [add(t, both_sides(t, 2, 1)) for t in tall]


def line_pair(v, g, w, scale, parity, order, step):
    a, b = order[0], order[1]
    first = parity == a
    h = add(g, w)
    u = add(w, v)
    q = add(w, h * scale)
    if u is None:
        return add(h, both_sides(jnp.where(first, q, 0.0), 2, step)) * scale
    m = jnp.where(first, q, u)
    second = add(edge_some(m, 2, step, 2.0, 1.0, True, True), both_sides(m, 2, 2 * step)) * scale
    if len(order) == 2:
        return add(h, both_sides(m, 2, step), jnp.where(first, 0.0, second)) * scale
    here, there = (-step, step) if a == 0 else (step, -step)
    index = lax.broadcasted_iota(jnp.int32, scale.shape, 2)
    ends = (index < 2 * step) | (index >= scale.shape[2] - 2 * step)
    square = scale * scale
    some = square * u
    m_here = jnp.where(first, q, q + some * jnp.where(ends, F32(2.0), F32(3.0)))
    m_there = jnp.where(first, q, q + some * F32(3.0))
    third = jnp.where(first, square * both_sides(u, 2, 3 * step), 0.0)
    return add(h, shift(m_here, 2, here), shift(m_there, 2, there), second, third) * scale


def phase1(v, g, zs, scale, steps):
    v = list(v)
    parity = lax.broadcasted_iota(jnp.int32, scale.shape, 2) % 2
    for yp, order in steps:
        w = add(zs[yp], pair_sum(add(zs[1 - yp], v[1 - yp]), yp, 1))
        v[yp] = line_pair(v[yp], g[yp], w, scale, parity, order, 1)
    return v


def phase2(v, g, zs, scale, steps):
    shape = scale.shape
    y_par = lax.broadcasted_iota(jnp.int32, shape, 1) % 2
    x_par = (lax.broadcasted_iota(jnp.int32, shape, 2) // 2) % 2
    for yp, order in steps:
        w = add(zs, both_sides(add(zs, v), 1, 1))
        new = line_pair(v, g, w, scale, x_par, order, 2)
        v = jnp.where(y_par == yp, new, 0.0 if v is None else v)
    return v


def chunks(low, high, size):
    for start in range(low, high, size):
        yield start, min(size, high - start)


YX = [(0, 0), (0, 1), (1, 0), (1, 1)]


NONE = [[None, None], [None, None]]


def run0(v, f, z0, z_count, odd, low, high, steps, fresh):
    for at, n in chunks(low, high, CHUNK0):
        here = pl.ds(at, n)
        below, above = (pl.ds(at, n), pl.ds(at + 1, n)) if odd else (pl.ds(at - 1, n), pl.ds(at, n))
        rhs = [[f[odd][yp, xp, here] for xp in (0, 1)] for yp in (0, 1)]
        scale = scale_rows(rhs[0][0].shape, z0 + 2 * at - LOW0 + odd, z_count)
        zs, old = NONE, NONE
        if fresh > 0:
            zs = [[v[1 - odd][yp, xp, below] + v[1 - odd][yp, xp, above] for xp in (0, 1)] for yp in (0, 1)]
        if fresh > 1:
            old = [[v[odd][yp, xp, here] for xp in (0, 1)] for yp in (0, 1)]
        new = phase0(old, rhs, zs, scale, steps)
        for yp, xp in YX:
            v[odd][yp, xp, here] = new[yp][xp]


def run1(v, f, z0, z_count, odd, low, high, steps, fresh):
    for at, n in chunks(low, high, CHUNK1):
        here = pl.ds(at, n)
        below, above = (pl.ds(at, n), pl.ds(at + 1, n)) if odd else (pl.ds(at - 1, n), pl.ds(at, n))
        g = [f[odd, here, yp] for yp in (0, 1)]
        scale = scale_rows(g[0].shape, z0 + 2 * at - LOW1 + odd, z_count)
        zs, old = NONE[0], NONE[0]
        if fresh > 0:
            zs = [v[1 - odd][yp, below] + v[1 - odd][yp, above] for yp in (0, 1)]
        if fresh > 1:
            old = [v[odd][yp, here] for yp in (0, 1)]
        new = phase1(old, g, zs, scale, steps)
        for yp in (0, 1):
            v[odd][yp, here] = new[yp]


def permutation(size, inverse):
    half = size // 2
    wide = lax.broadcasted_iota(jnp.int32, (size, size), 0 if inverse else 1)
    tall = lax.broadcasted_iota(jnp.int32, (size, size), 1 if inverse else 0)
    source = jnp.where(wide < half, 2 * wide, 2 * (wide - half) + 1)
    return jnp.where(tall == source, F32(1.0), F32(0.0))


def when(condition, act):
    @pl.when(condition)
    def _():
        act()


def send_order(far, halves):
    order = [(dz, h) for dz in (0, far, -far) for h in reversed(range(halves))]
    return [(dz, h) for dz, h in order if dz != 0 or h != 0]


def receive_order(far, halves):
    order = [(dz, h) for h in range(halves) for dz in (0, -far, far)]
    return [(dz, h) for dz, h in order if dz != 0 or h != 0]


def kernel(
    gz_n, gy_n, rhs_hbm, sol_ref, res_ref, alpha_ref,
    flat, mine, plain, got, fe, fo, ve, vo, dbuf, f1, v1e, v1o, vc, part, parts, nat,
    ssem, r1, rr, s2, r2, r3, rs, rhs_ref, s5, token,
):
    gz, gy = lax.axis_index("gz"), lax.axis_index("gy")
    zl, yl, nx = rhs_ref.shape
    fetch = pltpu.make_async_copy(rhs_hbm, rhs_ref, s5)
    fetch.start()
    y2, x2 = yl // 2, nx // 2
    yc = y2 // 2
    zc = zl // 2
    z_count = gz_n * zl
    z0 = gz * zl
    f, v = (fe, fo), (ve, vo)
    v1 = (v1e, v1o)
    halves = gy_n // 2
    sibling = gy + 1 - 2 * lax.rem(gy, 2)

    def there(dz):
        return (gz + dz >= 0) & (gz + dz < gz_n)

    def when_there(dz, go):
        if dz == 0:
            go()
        else:
            when(there(dz), go)

    barrier = pltpu.get_barrier_semaphore()
    count = jnp.int32(0)
    greet = [(dz, 2 * h) for h in reversed(range(halves)) for dz in (-1, 1)] + [(-2, 0), (2, 0)] + [(0, dg) for dg in range(1, gy_n)]
    greet = [(dz, dg, gy) for dz, dg in greet] + [(dz, 2 * h, sibling) for h in range(1, halves) for dz in (-1, 1)]
    for dz, dg, base in greet:

        def go(dz=dz, dg=dg, base=base):
            pl.semaphore_signal(
                barrier, inc=1, device_id=(gz + dz, lax.rem(base + dg, gy_n)), device_id_type=MESH
            )

        when_there(dz, go)
        count = count + (1 if dz == 0 else there(dz).astype(jnp.int32))

    fetch.wait()
    lane = lax.broadcasted_iota(jnp.int32, (zl * yl, x2), 1)
    source = 2 * lax.rem(lane, x2 // 2)
    rows = rhs_ref[...].reshape(zl * yl, nx)
    for xp in (0, 1):
        left, right = (
            jnp.take_along_axis(rows[:, i : i + x2], source + xp, axis=1, mode="promise_in_bounds") for i in (0, x2)
        )
        flat[xp] = jnp.where(lane < x2 // 2, left, right)
    for z in range(zl):
        for yp, xp in YX:
            row = flat[xp, pl.ds(z * yl + yp, y2, stride=2), :]
            mine[z % 2, z // 2, (yp * 2 + xp) * y2 : (yp * 2 + xp + 1) * y2, :] = row
            plain[z, (yp * 2 + xp) * y2 : (yp * 2 + xp + 1) * y2, :] = row

    parts1 = [
        {1: (zc - 1, (-2,)), 0: (0, tuple(range(0, zl, 2))), -1: (0, (zl,))},
        {1: (zc - 1, (-1,)), 0: (0, tuple(range(1, zl, 2)))},
        {1: (zl - LOW0, tuple(range(-LOW0, -2))), -1: (1, tuple(range(zl + 1, WINDOW - LOW0)))},
    ]
    place_of, at = {}, 0
    for part_ in parts1:
        for dz, (_, zs) in part_.items():
            for z in zs:
                place_of[z] = at
                at += 1
    messages = [(k, dz, h) for k, part_ in enumerate(parts1) for dz in part_ for h in range(halves) if dz or h]
    mail = {m: i for i, m in enumerate(messages)}
    moves2 = {-2: (0, zc // 2, 7), -1: (0, zc // 2, 5), 1: (0, zc // 2, 1), 2: (zc // 2 - 1, 1, 0)}
    counts = (EVENS, ODDS)

    def rows(k, dz):
        zs = parts1[k][dz][1]
        return pl.ds(place_of[zs[0]], len(zs))

    def outgoing(k, dz):
        first, zs = parts1[k][dz]
        return (plain if k == 2 else mine.at[k]).at[pl.ds(first, len(zs))]

    for k in (0, 1):
        got[gy, rows(k, 0)] = mine[k]
    for k, part_ in enumerate(parts1):
        for dz, edge in ((1, 0), (-1, gz_n - 1)):
            if dz in part_:

                @pl.when(gz == edge)
                def _(k=k, dz=dz):
                    got[:, rows(k, dz)] = jnp.zeros((gy_n, len(parts1[k][dz][1])) + got.shape[2:], F32)

    def pass_token(round_):
        reach = 2 << round_
        for dz in (-reach, reach):
            when_there(dz, lambda dz=dz: pl.semaphore_signal(
                token.at[round_], inc=1, device_id=(gz + dz, gy), device_id_type=MESH
            ))

    def take_token(round_):
        reach = 2 << round_
        pl.semaphore_wait(token.at[round_], there(-reach).astype(jnp.int32) + there(reach).astype(jnp.int32))

    def each_parity(index, act):
        for parity in (0, 1):
            when(lax.rem(index, 2) == parity, lambda parity=parity: act(parity))

    def edges(act):
        when(gz == 0, lambda: act(0))
        when(gz == gz_n - 1, lambda: act(1))
        when((gz > 0) & (gz < gz_n - 1), lambda: act(None))

    def unpack(k, g):
        for dz in parts1[k]:
            for z in parts1[k][dz][1]:
                for j, (yp, xp) in enumerate(YX):
                    row = got[g, place_of[z], j * y2 : (j + 1) * y2, :]
                    f[z % 2][yp, xp, (z + LOW0) // 2, g * y2 : (g + 1) * y2, :] = row

    def direct(k, dz, h, owner):
        g = lax.rem(gy + 2 * h, gy_n)
        return pltpu.make_async_remote_copy(
            src_ref=outgoing(k, dz),
            dst_ref=got.at[g if owner else gy, rows(k, dz)],
            send_sem=ssem.at[0],
            recv_sem=r1.at[mail[k, dz, (halves - h) % halves if owner else h]],
            device_id=(gz - dz if owner else gz + dz, g),
            device_id_type=MESH,
        )

    def relay(k, dz, h):
        place = got.at[lax.rem(gy + 2 * h, gy_n), rows(k, dz)]
        return pltpu.make_async_remote_copy(
            src_ref=mine.at[k] if dz == 0 and h == 0 else place,
            dst_ref=place,
            send_sem=ssem.at[1],
            recv_sem=rr.at[k],
            device_id=(gz, sibling),
            device_id_type=MESH,
        )

    def wait_rows(sem, n):
        block = got.at[pl.ds(0, halves), pl.ds(0, n)]
        pltpu.make_async_copy(block, block, sem).wait()

    def send(ks):
        def starts(parity):
            far = -1 if parity == 0 else 1
            for k in ks:
                for dz, h in send_order(far, halves):
                    if dz in parts1[k]:
                        when_there(dz, lambda: direct(k, dz, h, False).start())
                if 0 in parts1[k]:
                    relay(k, 0, 0).start()

        each_parity(gz, starts)

    def forward(ks):
        def forwards(parity):
            far = 1 if parity == 0 else -1
            for k in ks:
                for i, (dz, h) in enumerate(receive_order(far, halves)):
                    if k == 0 and ks[0] == 0 and i == 1:
                        send((2,))

                    def go():
                        direct(k, dz, h, True).wait_recv()
                        relay(k, dz, h).start()

                    if dz in parts1[k]:
                        when_there(-dz, go)

        each_parity(gz, forwards)
        each_parity(gy, lambda parity: [unpack(k, g) for k in ks for g in range(parity, gy_n, 2)])

    def height(k, dz):
        return len(parts1[k][dz][1]) if dz in parts1[k] else 0

    def relayed(k):
        total = sum(height(k, dz) for dz in (-1, 0, 1))
        less = (height(k, 1), height(k, -1))
        edges(lambda edge: wait_rows(rr.at[k], total - (0 if edge is None else less[edge])))
        each_parity(gy, lambda parity: [unpack(k, g) for g in range(1 - parity, gy_n, 2)])

    def sent():
        up, down = (sum(height(k, dz) for k in range(3)) for dz in (1, -1))
        own_rows = zl - zl // halves
        edges(lambda edge: wait_rows(ssem.at[0], own_rows + (down if edge != 0 else 0) + (up if edge != 1 else 0)))
        edges(lambda edge: wait_rows(ssem.at[1], zl + (up if edge != 0 else 0) + (down if edge != 1 else 0)))

    rounds = max(gz_n - 2, 1).bit_length() - 1
    pl.semaphore_wait(barrier, count)
    own = LOW0 // 2
    last = own + zc
    send((0, 1))
    forward((0, 1))
    if rounds > 0:
        pass_token(0)
    relayed(0)
    run0(v, f, z0, z_count, 0, own - 1, last + 1, PHASE_A, 0)
    relayed(1)
    run0(v, f, z0, z_count, 1, own - 1, last, PHASE_B, 1)
    run0(v, f, z0, z_count, 0, own, last, PHASE_C, 2)

    here, below, above = pl.ds(own, zc), pl.ds(own - 1, zc), pl.ds(own, zc)
    s = [[ve[yp, xp, here] + vo[yp, xp, below] + vo[yp, xp, above] for xp in (0, 1)] for yp in (0, 1)]
    tall = [s[0][xp] + pair_sum(s[1][xp], 0, 1) for xp in (0, 1)]
    dbuf[...] = fe[0, 0, here] - (27.0 * ve[0, 0, here] - (tall[0] + pair_sum(tall[1], 0, 2)))
    half = gy_n * yc
    for z in range(zc):
        for yp in (0, 1):
            f1[z % 2, 3 + z // 2, yp] = dbuf[z, pl.ds(yp, half, stride=2), :]
    for edge, low, n in ((0, 0, 3), (1, 0, 1), (gz_n - 2, 7, 2), (gz_n - 1, 5, 4)):

        @pl.when(gz == edge)
        def _(low=low, n=n):
            f1[:, low : low + n] = jnp.zeros((2, n) + f1.shape[2:], F32)

    sender = lax.rem(gy, 2) == 1
    def near(zp, dz, target):
        first, n, to = moves2[dz]
        n = min(n, counts[zp] - to)
        return pltpu.make_async_remote_copy(
            src_ref=f1.at[zp, pl.ds(3 + first, n)], dst_ref=f1.at[zp, pl.ds(to, n)],
            send_sem=s2.at[zp], recv_sem=r2.at[zp],
            device_id=(gz + dz, target), device_id_type=MESH,
        )

    def send_near(parity):
        far = -1 if parity == 0 else 1
        for zp in (0, 1):
            for dz in (far, 2 * far, -2 * far, -far):
                when_there(dz, lambda: near(zp, dz, gy).start())

    def wait_near(sem, sign, zps, times):
        def take(missing):
            n = sum(min(moves2[dz][1], counts[zp] - moves2[dz][2]) for zp in zps for dz in moves2 if dz not in missing)
            block = f1.at[pl.ds(0, times), pl.ds(0, n)]
            pltpu.make_async_copy(block, block, sem).wait()

        low_side, high_side = (sign * 2, sign), (-sign * 2, -sign)
        when(gz == 0, lambda: take(low_side))
        when(gz == 1, lambda: take(low_side[:1]))
        when(gz == gz_n - 2, lambda: take(high_side[:1]))
        when(gz == gz_n - 1, lambda: take(high_side))
        when((gz > 1) & (gz < gz_n - 2), lambda: take(()))

    if rounds > 0:
        take_token(0)
    if rounds > 1:
        pass_token(1)
    each_parity(gz, send_near)
    forward((2,))
    relayed(2)
    for phase, odd, ranges in (
        (PHASE_A, 0, ((0, own - 1), (last + 1, EVENS))),
        (PHASE_B, 1, ((0, own - 1), (last, ODDS))),
        (PHASE_C, 0, ((1, own), (last, EVENS - 1))),
    ):
        for low, high in ranges:
            run0(v, f, z0, z_count, odd, low, high, phase, odd if phase is not PHASE_C else 2)
    sent()
    c0, c_count = gz * zc, gz_n * zc
    wait_near(r2.at[0], 1, (0,), 1)
    run1(v1, f1, c0, c_count, 0, 0, EVENS, PHASE_A, 0)
    wait_near(r2.at[1], 1, (1,), 1)
    run1(v1, f1, c0, c_count, 1, 0, ODDS, PHASE_B, 1)
    run1(v1, f1, c0, c_count, 0, 1, EVENS - 1, PHASE_C, 2)

    f2 = []
    for i in range(1, EVENS - 1):
        s = [v1e[yp, pl.ds(i, 1)] + v1o[yp, pl.ds(i - 1, 1)] + v1o[yp, pl.ds(i, 1)] for yp in (0, 1)]
        tall = s[0] + pair_sum(s[1], 0, 1)
        f2.append(f1[0, pl.ds(i, 1), 0] - (27.0 * v1e[0, pl.ds(i, 1)] - (tall + both_sides(tall, 2, 1))))
    q0, q_count = gz * (zc // 2), gz_n * (zc // 2)
    f2e, f2o = f2[0::2], f2[1::2]
    scale2 = [scale_rows(f2[0].shape, q0 - LOW2 + i, q_count) for i in range(7)]
    even2 = [phase2(None, f2e[k], None, scale2[2 * k], PHASE_A) for k in range(4)]
    odd2 = [phase2(None, f2o[k], even2[k] + even2[k + 1], scale2[2 * k + 1], PHASE_B) for k in range(3)]
    for k in (1, 2):
        even2[k] = phase2(even2[k], f2e[k], odd2[k - 1] + odd2[k], scale2[2 * k], PHASE_C)
    v2 = [odd2[0], even2[1], odd2[1], even2[2], odd2[2]]
    in_lane = lax.broadcasted_iota(jnp.int32, v2[0].shape, 2) % 2 == 0
    for k in range(5):
        v1e[0, pl.ds(2 + k, 1)] = v1e[0, pl.ds(2 + k, 1)] + jnp.where(in_lane, v2[k], 0.0)

    run1(v1, f1, c0, c_count, 0, 2, 7, PHASE_A, 2)
    run1(v1, f1, c0, c_count, 1, 2, 6, PHASE_B, 2)
    run1(v1, f1, c0, c_count, 0, 3, 6, PHASE_C, 2)

    for c in range(-1, 6):
        odd = c % 2
        i = (c + LOW1 - odd) // 2
        for yp in (0, 1):
            vc[c + 1, pl.ds(yp, half, stride=2), :] = v1[odd][yp, i]
    ve[0, 0, pl.ds(1, 7)] = ve[0, 0, pl.ds(1, 7)] + vc[...]

    run0(v, f, z0, z_count, 0, 1, 8, PHASE_A, 2)
    run0(v, f, z0, z_count, 1, 1, 7, PHASE_B, 2)
    run0(v, f, z0, z_count, 0, 2, 7, PHASE_C, 2)

    numer = denom = None
    for odd in (0, 1):
        for k in range(zc):
            i = own + k
            here, below, above = pl.ds(i, 1), pl.ds(i - 1 + odd, 1), pl.ds(i + odd, 1)
            p = [[v[odd][yp, xp, here] for xp in (0, 1)] for yp in (0, 1)]
            s = [[p[yp][xp] + v[1 - odd][yp, xp, below] + v[1 - odd][yp, xp, above] for xp in (0, 1)] for yp in (0, 1)]
            b = box0(s)
            for yp, xp in YX:
                image = 27.0 * p[yp][xp] - b[yp][xp]
                numer = add(numer, f[odd][yp, xp, here] * p[yp][xp])
                denom = add(denom, p[yp][xp] * image)
                parity_at = k * 2 + odd
                nat[yp, xp, pl.ds(parity_at, 1)] = image
    rows = numer.shape[1]
    for j, total in enumerate((numer, denom)):
        acc = None
        for r in range(0, rows, 8):
            acc = add(acc, total[0, r : r + 8, :])
        part[pl.ds(j, 1), :] = jnp.sum(acc, axis=0, keepdims=True)

    for r in range(1, rounds):
        take_token(r)
        if r + 1 < rounds:
            pass_token(r + 1)

    def spread(to, target):
        return pltpu.make_async_remote_copy(
            src_ref=part, dst_ref=parts.at[gz], send_sem=rs, recv_sem=r3,
            device_id=(to, target), device_id_type=MESH,
        )

    @pl.when(sender)
    def _():
        for to in range(gz_n):

            def go():
                for g in (sibling, gy):
                    spread(to, g).start()

            when(gz != to, go)

    parts[gz] = part[...]

    back = permutation(nx, True)
    for which, out in ((0, sol_ref), (1, res_ref)):
        for z in range(zl):
            for yp, xp in YX:
                if which == 0:
                    row = v[z % 2][yp, xp, own + z // 2, pl.ds(gy * y2, y2), :]
                else:
                    row = nat[yp, xp, z, pl.ds(gy * y2, y2), :]
                flat[xp, pl.ds(z * yl + yp, y2, stride=2), :] = row
        out[...] = jnp.dot(
            jnp.concatenate([flat[0], flat[1]], axis=1), back, precision=lax.Precision.HIGHEST, preferred_element_type=F32
        ).reshape(zl, yl, nx)

    others = parts.at[pl.ds(0, gz_n - 1)]
    pltpu.make_async_copy(others, others, r3).wait()
    [wait_near(s2.at[zp], -1, (zp,), 1) for zp in (0, 1)]
    when(sender, lambda: [pltpu.make_async_copy(others, others, rs).wait() for _ in range(2)])
    sums = parts[0]
    for d in range(1, gz_n):
        sums = sums + parts[d]
    alpha = jnp.sum(sums[0:1], axis=1, keepdims=True) / jnp.sum(sums[1:2], axis=1, keepdims=True)
    alpha_ref[...] = jnp.broadcast_to(alpha.reshape(1, 1), alpha_ref.shape)


def solution(mesh):
    gz_n, gy_n = mesh.shape["gz"], mesh.shape["gy"]

    def body(rhs):
        zl, yl, nx = rhs.shape
        y2, x2 = yl // 2, nx // 2
        y_half = gy_n * y2
        zc, yc = zl // 2, y2 // 2
        vmem = lambda *shape: pltpu.VMEM(shape, F32)
        dma = lambda *shape: pltpu.SemaphoreType.DMA(shape)
        p, image, alpha = pl.pallas_call(
            functools.partial(kernel, gz_n, gy_n),
            out_shape=[vmem(*rhs.shape)] * 2 + [vmem(yl, nx)],
            in_specs=[pl.BlockSpec(memory_space=pl.ANY)],
            out_specs=[pl.BlockSpec(memory_space=pltpu.VMEM)] * 3,
            scratch_shapes=[
                vmem(2, zl * yl, x2),
                vmem(2, zc, 4 * y2, x2),
                vmem(zl, 4 * y2, x2),
                vmem(gy_n, WINDOW, 4 * y2, x2),
                vmem(2, 2, EVENS, y_half, x2),
                vmem(2, 2, ODDS, y_half, x2),
                vmem(2, 2, EVENS, y_half, x2),
                vmem(2, 2, ODDS, y_half, x2),
                vmem(zc, y_half, x2),
                vmem(2, EVENS, 2, gy_n * yc, x2),
                vmem(2, EVENS, gy_n * yc, x2),
                vmem(2, ODDS, gy_n * yc, x2),
                vmem(7, y_half, x2),
                vmem(2, x2),
                vmem(gz_n, 2, x2),
                vmem(2, 2, zl, y_half, x2),
                dma(2), dma(7 * (gy_n // 2) - 2), dma(3), dma(2), dma(2),
                pltpu.SemaphoreType.DMA, pltpu.SemaphoreType.DMA,
                vmem(zl, yl, nx), pltpu.SemaphoreType.DMA,
                pltpu.SemaphoreType.REGULAR((max(1, max(gz_n - 2, 1).bit_length() - 1),)),
            ],
            compiler_params=pltpu.CompilerParams(has_side_effects=True, collective_id=0),
        )(rhs)
        return p * alpha, rhs - image * alpha

    return jax.shard_map(
        lambda rhs: tuple(body(rhs)),
        mesh=mesh,
        in_specs=(P("gz", "gy", None),),
        out_specs=(P("gz", "gy", None), P("gz", "gy", None)),
        check_vma=False,
    )
```
